256 devices in a mesh: plane: 64 (over x, z, core), depth: 4 (over y).
Axes of the slice: x: 4, y: 4, z: 8, core: 2. Of those that a mesh axis runs over, the one named last changes fastest.
Arguments:
- labels: int32 [256, 64, 384], P('plane', 'depth'), may hold values from 0 to 3
- start: int32 [3, 16, 256, 64, 384], P(None, None, 'plane', 'depth'), may hold values from -8 to 8
Outputs:
- basis_cols: float32 [80, 256, 64, 384], P(None, 'plane', 'depth')
- coords: float32 [3, 80, 48], replicated
The draws below stay inside these ranges and needn't reach their ends.
All inputs are finite; a program needn't handle non-finite values.
Results may differ from the reference program's by a relative error of at most 0.00016.
Values sent between devices are 32-bit elements; how exact they have to be, the bound alone decides.
No kernel may reach another device: no remote copies, remote signals or barrier semaphores. Data moves between devices by JAX's collectives and lax.ppermute only.
A program may use at most 64 MiB of HBM per device.

```python
import jax
import jax.numpy as jnp
from jax import lax

CZ = 384
B = 16
STEPS = 2
REGIONS = 4
NX = 256
NY = 64


def place_ends(array, own_key, low, largest):
    index_at = [jax.random.randint(jax.random.fold_in(own_key, axis), (), 0, length) for axis, length in enumerate(array.shape)]
    longest = array.shape.index(max(array.shape))
    neighbour = index_at[:longest] + [(index_at[longest] + 1) % array.shape[longest]] + index_at[longest + 1:]
    return array.at[tuple(index_at)].set(low).at[tuple(neighbour)].set(largest)


def setup_inputs(seed: int = 0) -> dict:
    splits = jax.random.split(jax.random.key(seed), 3)
    return {
        "labels": place_ends(jax.random.randint(splits[0], (NX, NY, CZ), 0, REGIONS), jax.random.fold_in(splits[0], 1), 0, REGIONS - 1).astype(jnp.int32),
        "start": place_ends(jax.random.randint(splits[1], (3, B, NX, NY, CZ), -8, 9), jax.random.fold_in(splits[1], 1), -8, 8).astype(jnp.int32),
    }


highest = lax.Precision.HIGHEST
permittivity_table = (1.0, 2.5, 4.0, 6.5)
damping_table = (0.3, 1.2, 0.05, 2.0)
outer_table = (1.0, 0.5, 2.0, 0.8)
inner_table = (1.0, 3.0, 0.6, 1.5)

def lookup(labels, table):
    result = jnp.zeros(labels.shape, jnp.float32)
    for region, entry_value in enumerate(table):
        result = result + entry_value * (labels == region).astype(jnp.float32)
    return result

def combine(fields, matrix):
    return jnp.einsum('acde,ab->bcde', fields, matrix, precision=highest)

def inner_sum(left_side, right_side):
    return jnp.einsum('acde,bcde->ab', left_side, right_side, precision=highest)

def inverse_factor(gram_mean):
    factor = jnp.linalg.cholesky(gram_mean)
    eye_matrix = jnp.eye(gram_mean.shape[0], dtype=jnp.float32)
    return (factor, jax.scipy.linalg.solve_triangular(factor, eye_matrix, lower=True))

def normalize(column):
    small_gram = jnp.einsum('iab,iac->bc', column, column, precision=highest)
    factor, inverse = inverse_factor(small_gram)
    return jnp.einsum('iab,bc->iac', column, inverse.T, precision=highest)

def extend_coords(coords, newest, projected, factor):
    block_size = newest.shape[2]
    padding = jnp.zeros((3, block_size, coords.shape[2]), jnp.float32)
    widened = jnp.concatenate([coords, padding], axis=1)
    square = jnp.zeros((block_size, block_size), jnp.float32)
    column = jnp.stack([jnp.concatenate([projected, factor.T], 0), jnp.concatenate([newest[0], square], 0), jnp.concatenate([newest[1], square], 0)])
    for sweep_index in range(2):
        against = jnp.einsum('iab,iac->bc', widened, column, precision=highest)
        column = column - jnp.einsum('iab,bc->iac', widened, against, precision=highest)
    return jnp.concatenate([widened, normalize(column)], axis=2)

def laplace(fields):
    padded = jnp.pad(fields, ((0, 0), (1, 1), (1, 1), (1, 1)))
    center = padded[:, 1:-1, 1:-1, 1:-1]
    beside = padded[:, 2:, 1:-1, 1:-1] + padded[:, :-2, 1:-1, 1:-1]
    beside = beside + padded[:, 1:-1, 2:, 1:-1] + padded[:, 1:-1, :-2, 1:-1]
    beside = beside + padded[:, 1:-1, 1:-1, 2:] + padded[:, 1:-1, 1:-1, :-2]
    return 6.0 * center - beside

def reference(labels, start):
    cells_total = NX * NY * CZ
    permittivity = lookup(labels, permittivity_table)
    damping = lookup(labels, damping_table)
    outer_coef = lookup(labels, outer_table)
    inner_coef = lookup(labels, inner_table)
    stacked = start.reshape(3 * B, NX, NY, CZ).astype(jnp.float32)
    factor, inverse = inverse_factor(inner_sum(stacked, stacked) / cells_total)
    basis_cols = combine(stacked, inverse.T)
    coords = normalize(jnp.transpose(factor.T.reshape(3 * B, 3, B), (1, 0, 2)))
    for section in range(STEPS):
        newest = coords[:, :, coords.shape[2] - B:]
        part_one = combine(basis_cols, newest[0])
        part_two = combine(basis_cols, newest[1])
        part_three = combine(basis_cols, newest[2])
        lifted = -(outer_coef * laplace(part_one) + damping * part_two + inner_coef * laplace(part_three)) / permittivity
        projected = inner_sum(basis_cols, lifted) / cells_total
        residual = lifted - combine(basis_cols, projected)
        factor, inverse = inverse_factor(inner_sum(residual, residual) / cells_total)
        fresh_cols = combine(residual, inverse.T)
        coords = extend_coords(coords, newest, projected, factor)
        basis_cols = jnp.concatenate([basis_cols, fresh_cols], 0)
    return (basis_cols, coords)
```

```python
import jax
import jax.numpy as jnp
from jax import lax
from jax.sharding import Mesh
from jax.sharding import PartitionSpec as P

PLANE = ("plane_0", "plane_1", "plane_2")
WIDE = ("plane_1", "depth")
NARROW = ("plane_0", "plane_2")
B = 16

highest = lax.Precision.HIGHEST
permittivity_table = (1.0, 2.5, 4.0, 6.5)
damping_table = (0.3, 1.2, 0.05, 2.0)
outer_table = (1.0, 0.5, 2.0, 0.8)
inner_table = (1.0, 3.0, 0.6, 1.5)


def sum_over(value, axes):
    peers = lax.axis_size(axes)
    copies = jnp.broadcast_to(value[None], (peers,) + value.shape)
    return jnp.sum(lax.all_to_all(copies, axes, 0, 0, tiled=True), axis=0)


def sum_all(value):
    return sum_over(sum_over(value, WIDE), NARROW)


def shift(edge, axis, step):
    peers = lax.axis_size(axis)
    pairs = [(i, i + step) for i in range(peers) if 0 <= i + step < peers]
    return lax.ppermute(edge, axis, pairs)


def halos(fields):
    return (
        shift(fields[:, -1:], PLANE, 1),
        shift(fields[:, :1], PLANE, -1),
        shift(fields[:, :, -1:], "depth", 1),
        shift(fields[:, :, :1], "depth", -1),
    )


def laplace(fields, edges):
    below, above, before, behind = [edge.astype(jnp.float32) for edge in edges]
    deeper = jnp.pad(fields, ((0, 0), (0, 0), (0, 0), (1, 1)))
    across = jnp.concatenate([below, fields, above], axis=1)
    along = jnp.concatenate([before, fields, behind], axis=2)
    beside = across[:, 2:] + across[:, :-2] + along[:, :, 2:] + along[:, :, :-2]
    return 6.0 * fields - (beside + deeper[..., 2:] + deeper[..., :-2])


def lookup(labels, table):
    result = jnp.zeros(labels.shape, jnp.float32)
    for region, entry_value in enumerate(table):
        result = result + entry_value * (labels == region).astype(jnp.float32)
    return result


def small(spec, *terms):
    return jnp.einsum(spec, *terms, precision=highest)


def split(values):
    high = lax.reduce_precision(values, 8, 7)
    return high.astype(jnp.bfloat16), (values - high).astype(jnp.bfloat16)


def combine(fields, matrix):
    high, low = split(matrix)
    both = jnp.concatenate([high, low], axis=1)
    out = jnp.einsum("acde,ab->bcde", fields, both, preferred_element_type=jnp.float32)
    return out[: matrix.shape[1]] + out[matrix.shape[1] :]


def inverse_factor(gram_mean):
    factor = jnp.linalg.cholesky(gram_mean)
    eye_matrix = jnp.eye(gram_mean.shape[0], dtype=jnp.float32)
    return (factor, jax.scipy.linalg.solve_triangular(factor, eye_matrix, lower=True))


def normalize(column):
    factor, inverse = inverse_factor(small("iab,iac->bc", column, column))
    return small("iab,bc->iac", column, inverse.T)


def extend_coords(coords, newest, projected, factor):
    padding = jnp.zeros((3, B, coords.shape[2]), jnp.float32)
    widened = jnp.concatenate([coords, padding], axis=1)
    square = jnp.zeros((B, B), jnp.float32)
    column = jnp.stack(
        [
            jnp.concatenate([projected, factor.T], 0),
            jnp.concatenate([newest[0], square], 0),
            jnp.concatenate([newest[1], square], 0),
        ]
    )
    for sweep_index in range(2):
        against = small("iab,iac->bc", widened, column)
        column = column - small("iab,bc->iac", widened, against)
    return jnp.concatenate([widened, normalize(column)], axis=2)


def products(spanning, high, low):
    rows = jnp.concatenate([spanning, high, low], axis=0)
    cols = jnp.concatenate([high, low], axis=0)
    table = jnp.einsum("acde,bcde->ab", rows, cols, preferred_element_type=jnp.float32)
    table = table[:, :B] + table[:, B:]
    count = spanning.shape[0]
    return jnp.concatenate([table[:count], table[count : count + B] + table[count + B :]], 0)


def sum_table(table):
    packed = table.reshape(-1, 128)
    return sum_all(packed).reshape(table.shape)


def per_device(labels, start):
    cells_total = labels.size * lax.axis_size(PLANE) * lax.axis_size("depth")
    permittivity = lookup(labels, permittivity_table)
    outer_coef = -lookup(labels, outer_table) / permittivity
    damping = -lookup(labels, damping_table) / permittivity
    inner_coef = -lookup(labels, inner_table) / permittivity
    whole = start.reshape((3 * B,) + labels.shape)
    edges = halos(whole)
    fields = whole.astype(jnp.bfloat16)
    local = jnp.einsum("acde,bcde->ab", fields, fields, preferred_element_type=jnp.float32)
    factor, inverse = inverse_factor(sum_table(local) / cells_total)
    coords = normalize(jnp.transpose(factor.T.reshape(3 * B, 3, B), (1, 0, 2)))
    applied = laplace(whole.astype(jnp.float32), edges).astype(jnp.bfloat16)
    to_basis = inverse.T

    newest = coords
    weights = small("ab,ibc->iac", to_basis, newest)
    from_applied = combine(applied, jnp.concatenate([weights[0], weights[2]], 1))
    lifted = (
        outer_coef * from_applied[:B]
        + damping * combine(fields, weights[1])
        + inner_coef * from_applied[B:]
    )
    high, low = split(lifted)
    edges = halos(lifted)
    table = sum_table(products(fields, high, low)) / cells_total
    projected = small("ab,ac->bc", to_basis, table[: 3 * B])
    gram_mean = table[3 * B :] - small("ab,ac->bc", projected, projected)
    factor, inverse = inverse_factor(gram_mean)
    coords = extend_coords(coords, newest, projected, factor)
    fresh_start = -small("ab,bc,dc->ad", to_basis, projected, inverse)
    to_basis = jnp.concatenate(
        [
            jnp.concatenate([to_basis, fresh_start], 1),
            jnp.concatenate([jnp.zeros((B, 3 * B), jnp.float32), inverse.T], 1),
        ],
        0,
    )
    spanning = jnp.concatenate([fields, high, low], 0)
    lifted_applied = laplace(lifted, edges)
    high_applied, low_applied = split(lifted_applied)
    spanning_applied = jnp.concatenate([applied, high_applied, low_applied], 0)

    def both(matrix):
        return jnp.concatenate([matrix, matrix[3 * B :]], 0)

    newest = coords[:, :, coords.shape[2] - B :]
    weights = small("ab,ibc->iac", to_basis, newest)
    from_applied = combine(spanning_applied, both(jnp.concatenate([weights[0], weights[2]], 1)))
    second = (
        outer_coef * from_applied[:B]
        + damping * combine(spanning, both(weights[1]))
        + inner_coef * from_applied[B:]
    )
    high, low = split(second)
    table = products(spanning, high, low)
    count = 3 * B
    table = jnp.concatenate([table[:count], table[count : count + B] + table[count + B : count + 2 * B], table[count + 2 * B :]], 0)
    table = sum_table(table) / cells_total
    projected = small("ab,ac->bc", to_basis, table[: 4 * B])
    gram_mean = table[4 * B :] - small("ab,ac->bc", projected, projected)
    factor, inverse = inverse_factor(gram_mean)
    coords = extend_coords(coords, newest, projected, factor)
    fresh_start = -small("ab,bc,dc->ad", to_basis, projected, inverse)
    final = jnp.concatenate([to_basis, fresh_start], 1)
    last = jnp.concatenate([jnp.zeros((B, 4 * B), jnp.float32), inverse.T], 1)
    matrix = jnp.concatenate([both(final), last, last], 0)
    basis_cols = combine(jnp.concatenate([spanning, high, low], 0), matrix)
    return (basis_cols, coords)


def solution(mesh):
    finer = Mesh(
        mesh.devices.reshape(4, 8, 2, mesh.shape["depth"]),
        ("plane_0", "plane_1", "plane_2", "depth"),
    )
    return jax.shard_map(
        per_device,
        mesh=finer,
        in_specs=(P(PLANE, "depth", None), P(None, None, PLANE, "depth", None)),
        out_specs=(P(None, PLANE, "depth", None), P()),
        check_vma=False,
    )
```

```python
import jax
import jax.numpy as jnp
from jax import lax
from jax.experimental import pallas as pl
from jax.experimental.pallas import tpu as pltpu
from jax.sharding import Mesh
from jax.sharding import PartitionSpec as P

PLANE = ("plane_0", "plane_1", "plane_2")
WIDE = ("plane_1", "depth")
NARROW = ("plane_0", "plane_2")
B = 16
S = 3 * B
V = 5 * B
A = V + 2 * B

f32 = jnp.float32
bf16 = jnp.bfloat16
highest = lax.Precision.HIGHEST
permittivity_table = (1.0, 2.5, 4.0, 6.5)
damping_table = (0.3, 1.2, 0.05, 2.0)
outer_table = (1.0, 0.5, 2.0, 0.8)
inner_table = (1.0, 3.0, 0.6, 1.5)
CHAIN = ((0, 3, 4), (1, 0, 3), (2, 1, 0))

VMEM = pltpu.VMEM
ANY = pl.ANY


def sum_over(value, axes):
    peers = lax.axis_size(axes)
    copies = jnp.broadcast_to(value[None], (peers,) + value.shape)
    return jnp.sum(lax.all_to_all(copies, axes, 0, 0, tiled=True), axis=0)


def shift(edge, axis, step):
    peers = lax.axis_size(axis)
    pairs = [(i, i + step) for i in range(peers) if 0 <= i + step < peers]
    return lax.ppermute(edge, axis, pairs)


def exchange(low, high, front, back):
    return (
        shift(high, PLANE, 1),
        shift(low, PLANE, -1),
        shift(back, "depth", 1),
        shift(front, "depth", -1),
    )


def call(body, outs, operands, scratch=(), limit=16):
    specs, shapes, results = [], [], []
    for operand, space in operands:
        specs.append(pl.BlockSpec(memory_space=space))
        results.append(operand if space is pl.ANY else pltpu.with_memory_space_constraint(operand, space))
    out_specs = []
    for shape, kind, space in outs:
        out_specs.append(pl.BlockSpec(memory_space=space))
        shapes.append(jax.ShapeDtypeStruct(shape, kind) if space is pl.ANY else space(shape, kind))
    return pl.pallas_call(
        body,
        out_shape=tuple(shapes),
        in_specs=specs,
        out_specs=tuple(out_specs),
        scratch_shapes=list(scratch),
        compiler_params=pltpu.CompilerParams(vmem_limit_bytes=limit * 2**20),
    )(*results)


def sweep(px, py, step, carry):
    for p in range(px):
        carry = step(p, 0, carry)
        carry = lax.fori_loop(1, py - 1, lambda y, value, p=p: step(p, y, value), carry)
        carry = step(p, py - 1, carry)
    return carry


def read_start(start, px, py, cz):
    halves = py // 8

    def body(start_ref, fields_ref, low_ref, high_ref, front_ref, back_ref, raw, sems):
        def copy(chunk):
            p, h = chunk // halves, chunk % halves
            return pltpu.make_async_copy(start_ref.at[:, p, pl.ds(8 * h, 8), :], raw.at[chunk], sems.at[chunk])

        for chunk in range(px * halves):
            copy(chunk).start()

        def step(chunk, carry):
            copy(chunk).wait()
            p, h = chunk // halves, chunk % halves
            rows = pl.multiple_of(8 * h, 8)
            turned = jnp.swapaxes(raw[chunk].astype(f32), 0, 1)
            fields_ref[p, pl.ds(rows, 8)] = turned.astype(bf16)

            @pl.when(p == 0)
            def _():
                low_ref[pl.ds(rows, 8)] = turned

            @pl.when(p == px - 1)
            def _():
                high_ref[pl.ds(rows, 8)] = turned

            @pl.when(h == 0)
            def _():
                front_ref[p] = turned[0]

            @pl.when(h == halves - 1)
            def _():
                back_ref[p] = turned[7]

            return carry

        lax.fori_loop(0, px * halves, step, 0)

    plane, row = ((py, S, cz), f32, VMEM), ((px, S, cz), f32, VMEM)
    return call(
        body,
        (((px, py, S, cz), bf16, VMEM), plane, plane, row, row),
        ((start, pltpu.HBM),),
        (pltpu.VMEM((px * halves, S, 8, cz), jnp.int32), pltpu.SemaphoreType.DMA((px * halves,))),
    )


def laplace(inside, edges, p, y, at, px, py, cz):
    below, above, before, behind = edges
    kept = slice(at, at + B)

    def get(p, y):
        if p < 0:
            row = below[y, kept]
        elif p == px:
            row = above[y, kept]
        elif isinstance(y, int) and y < 0:
            row = before[p, kept]
        elif isinstance(y, int) and y == py:
            row = behind[p, kept]
        else:
            row = inside[p, y, kept]
        return row.astype(f32)

    center = get(p, y)
    lane = lax.broadcasted_iota(jnp.int32, (B, cz), 1)
    left = jnp.where(lane == 0, 0.0, pltpu.roll(center, 1, 1))
    right = jnp.where(lane == cz - 1, 0.0, pltpu.roll(center, cz - 1, 1))
    beside = (get(p + 1, y) + get(p - 1, y)) + (get(p, y + 1) + get(p, y - 1)) + (left + right)
    return 6.0 * center - beside


def set_coefs(labels_ref, coefs, px):
    for p in range(px):
        labels = labels_ref[p]
        for which, table in enumerate((outer_table, damping_table, inner_table)):
            values = [-entry / eps for entry, eps in zip(table, permittivity_table)]
            result = jnp.full(labels.shape, values[0], f32)
            for region in range(1, 4):
                result = jnp.where(labels == region, values[region], result)
            coefs[which, p] = result


def first_lift(labels, fields, edges, px, py, cz):
    def body(labels_ref, fields_ref, below, above, before, behind, lifted, low, high, front, back, coefs):
        set_coefs(labels_ref, coefs, px)
        around = (below, above, before, behind)

        def step(p, y, carry):
            outer, damping, inner = [coefs[k, p, pl.ds(y, 1), :] for k in range(3)]
            out = (
                outer * laplace(fields_ref, around, p, y, 0, px, py, cz)
                + damping * fields_ref[p, y, B : 2 * B, :].astype(f32)
                + inner * laplace(fields_ref, around, p, y, 2 * B, px, py, cz)
            )
            lifted[p, y] = out
            if p == 0:
                low[y] = out
            if p == px - 1:
                high[y] = out
            if isinstance(y, int):
                (back if y else front)[p] = out
            return carry

        sweep(px, py, step, 0)

    plane, row = ((py, B, cz), f32, VMEM), ((px, B, cz), f32, VMEM)
    return call(
        body,
        (((px, py, B, cz), f32, VMEM), plane, plane, row, row),
        ((labels, VMEM), (fields, VMEM)) + tuple((edge, VMEM) for edge in edges),
        (pltpu.VMEM((3, px, py, cz), f32),),
        4,
    )


def second_lift(labels, fields, edges, lifted, ends, px, py, cz):
    def body(labels_ref, fields_ref, lifted_ref, *refs):
        edge_refs, end_refs, (parts, packed, coefs) = refs[:4], refs[4:8], refs[8:]
        set_coefs(labels_ref, coefs, px)

        def step(p, y, gram):
            outer, damping, inner = [coefs[k, p, pl.ds(y, 1), :] for k in range(3)]
            now = fields_ref[p, y]
            second = (
                outer * laplace(lifted_ref, end_refs, p, y, 0, px, py, cz)
                + damping * now[:B].astype(f32)
                + inner * laplace(fields_ref, edge_refs, p, y, B, px, py, cz)
            )
            both = jnp.concatenate([lifted_ref[p, y], second], 0)
            high = both.astype(bf16)
            low = (both - high.astype(f32)).astype(bf16)
            every = jnp.concatenate([now, high, low], 0)
            parts[p, y] = every
            return gram + lax.dot_general(every, every, (((1,), (1,)), ((), ())), preferred_element_type=f32)

        gram = sweep(px, py, step, jnp.zeros((A, A), f32))
        gram = jnp.concatenate([gram, jnp.zeros((A, 128 - A), f32)], 1)
        gram = jnp.concatenate([gram[:S], gram[S:V] + gram[V:]], 0)
        lane = lax.broadcasted_iota(jnp.int32, (V, 128), 1)
        low = pltpu.roll(gram, 128 - 2 * B, 1)
        gram = gram + jnp.where((lane >= S) & (lane < V), low, 0.0)
        half = V // 2
        lane = lax.broadcasted_iota(jnp.int32, (half, 128), 1)
        packed[...] = jnp.where(lane < V, gram[half:], pltpu.roll(gram[:half], V, 1))

    return call(
        body,
        (((px, py, A, cz), bf16, VMEM), ((V // 2, 128), f32, VMEM)),
        ((labels, VMEM), (fields, VMEM), (lifted, VMEM)) + tuple((edge, VMEM) for edge in edges + ends),
        (pltpu.VMEM((3, px, py, cz), f32),),
        4,
    )


def factorize(matrix, count):
    lane = lax.broadcasted_iota(jnp.int32, (8, 128), 1)
    sub = lax.broadcasted_iota(jnp.int32, (8, 128), 0)
    tiles = [matrix[8 * j : 8 * j + 8] for j in range(count // 8)]
    right = [jnp.where(lane == sub + 8 * j, 1.0, 0.0) for j in range(count // 8)]
    upper, inverse = [], []
    for k in range(count):
        own, s = k // 8, k % 8
        pivot = tiles[own][s : s + 1, k : k + 1]
        scale = lax.rsqrt(pivot)
        row = tiles[own][s : s + 1] * scale
        other = right[own][s : s + 1] * scale
        upper.append(row)
        inverse.append(other)
        for j in range(own, count // 8):
            factor = tiles[j][:, k : k + 1] * scale
            if j == own:
                factor = jnp.where(sub[:, :1] > s, factor, 0.0)
            tiles[j] = tiles[j] - factor * row
            right[j] = right[j] - factor * other
    upper = jnp.concatenate(upper, 0)
    inverse = jnp.concatenate(inverse, 0)
    lane = lax.broadcasted_iota(jnp.int32, (count, 128), 1)
    sub = lax.broadcasted_iota(jnp.int32, (count, 128), 0)
    return jnp.where((lane >= sub) & (lane < count), upper, 0.0), inverse


def algebra(packed, cells_total):
    half = V // 2

    def body(packed_ref, matrix_ref, coords_ref):
        table = packed_ref[...] * (1.0 / cells_total)
        turned = jnp.concatenate([table, jnp.zeros((128 - half, 128), f32)], 0).T
        first = jnp.concatenate([pltpu.roll(table, 128 - V, 1), table], 0)
        lane = lax.broadcasted_iota(jnp.int32, (V, 128), 1)
        gram = jnp.where(lane < half, first, jnp.where(lane < V, pltpu.roll(turned[:V], half, 1), 0.0))
        lane = lax.broadcasted_iota(jnp.int32, (B, 128), 1)
        rows = []
        for i in range(3):
            total = jnp.zeros((B, 128), f32)
            for blocks in CHAIN:
                strip = gram[B * blocks[i] : B * blocks[i] + B]
                for j in range(3):
                    moved = pltpu.roll(strip, (B * (j - blocks[j])) % 128, 1)
                    total = total + jnp.where((lane >= B * j) & (lane < B * j + B), moved, 0.0)
            rows.append(total)
        upper, inverse = factorize(gram, V)
        _, small = factorize(jnp.concatenate(rows, 0), S)
        small = jnp.concatenate([small, jnp.zeros((128 - S, 128), f32)], 0).T
        for i in range(3):
            pieces = [jnp.zeros((B, 128), f32)] * 8
            for j in range(3):
                pieces[CHAIN[i][j]] = small[B * j : B * j + B]
            coords = jnp.dot(upper, jnp.concatenate(pieces, 0), precision=highest, preferred_element_type=f32)
            coords_ref[i] = coords[:, :S]
        lane = lax.broadcasted_iota(jnp.int32, (V, 128), 1)
        matrix = jnp.where(lane < V, inverse, pltpu.roll(inverse, 2 * B, 1))[:, :A]
        high = matrix.astype(bf16)
        matrix_ref[:V] = high
        matrix_ref[V:] = (matrix - high.astype(f32)).astype(bf16)

    return call(
        body,
        (((2 * V, A), bf16, VMEM), ((3, V, S), f32, VMEM)),
        ((packed, VMEM),),
        limit=4,
    )


def write_basis(parts, matrix, px, py, cz):
    halves = py // 8

    def body(parts_ref, matrix_ref, out_ref, turned, ready, sems):
        weights = matrix_ref[...]

        def copy(chunk):
            p, h = chunk // halves, chunk % halves
            return pltpu.make_async_copy(ready.at[chunk], out_ref.at[:, p, pl.ds(8 * h, 8), :], sems.at[chunk])

        def step(chunk, carry):
            p, h = chunk // halves, chunk % halves
            for y in range(8):
                out = jnp.dot(weights, parts_ref[p, 8 * h + y], preferred_element_type=f32)
                turned[y] = out[:V] + out[V:]
            ready[chunk] = jnp.swapaxes(turned[...], 0, 1)
            copy(chunk).start()
            return carry

        lax.fori_loop(0, px * halves, step, 0)
        for chunk in range(px * halves):
            copy(chunk).wait()

    return call(
        body,
        (((V, px, py, cz), f32, ANY),),
        ((parts, VMEM), (matrix, VMEM)),
        (
            pltpu.VMEM((8, V, cz), f32),
            pltpu.VMEM((px * halves, V, 8, cz), f32),
            pltpu.SemaphoreType.DMA((px * halves,)),
        ),
        20,
    )[0]


def per_device(labels, start):
    px, py, cz = labels.shape
    cells_total = labels.size * lax.axis_size(PLANE) * lax.axis_size("depth")
    fields, *edges = read_start(start.reshape((S, px, py, cz)), px, py, cz)
    edges = exchange(*edges)
    lifted, *ends = first_lift(labels, fields, edges, px, py, cz)
    ends = exchange(*ends)
    parts, packed = second_lift(labels, fields, edges, lifted, ends, px, py, cz)
    packed = sum_over(sum_over(packed, WIDE), NARROW)
    matrix, coords = algebra(packed, cells_total)
    return (write_basis(parts, matrix, px, py, cz), coords)


def solution(mesh):
    finer = Mesh(
        mesh.devices.reshape(4, 8, 2, mesh.shape["depth"]),
        ("plane_0", "plane_1", "plane_2", "depth"),
    )
    return jax.shard_map(
        per_device,
        mesh=finer,
        in_specs=(P(PLANE, "depth", None), P(None, None, PLANE, "depth", None)),
        out_specs=(P(None, PLANE, "depth", None), P()),
        check_vma=False,
    )
```

```python
import jax
import jax.numpy as jnp
from jax import lax
from jax.experimental import pallas as pl
from jax.experimental.pallas import tpu as pltpu
from jax.sharding import Mesh
from jax.sharding import PartitionSpec as P

PLANE = ("plane_0", "plane_1", "plane_2")
WIDE = ("plane_1", "depth")
B = 16
S = 3 * B
V = 5 * B
A = V + 2 * B

f32 = jnp.float32
bf16 = jnp.bfloat16
highest = lax.Precision.HIGHEST
permittivity_table = (1.0, 2.5, 4.0, 6.5)
damping_table = (0.3, 1.2, 0.05, 2.0)
outer_table = (1.0, 0.5, 2.0, 0.8)
inner_table = (1.0, 3.0, 0.6, 1.5)
CHAIN = ((0, 3, 4), (1, 0, 3), (2, 1, 0))
BLOCKS = [(i, j) for j in range(5) for i in range(j + 1)]

VMEM = pltpu.VMEM
ANY = pl.ANY


def sum_over(value, axes):
    peers = lax.axis_size(axes)
    copies = jnp.broadcast_to(value[None], (peers,) + value.shape)
    return jnp.sum(lax.all_to_all(copies, axes, 0, 0, tiled=True), axis=0)


def sum_all(table):
    both = jnp.sum(lax.all_gather(table, "plane_2"), axis=0)
    own = jnp.where(lax.axis_index("plane_2") == 0, both[:B], both[B:])
    own = sum_over(sum_over(own, WIDE), "plane_0")
    return lax.all_gather(own, "plane_2", tiled=True)


def shift(edge, axis, step):
    peers = lax.axis_size(axis)
    pairs = [(i, i + step) for i in range(peers) if 0 <= i + step < peers]
    return lax.ppermute(edge, axis, pairs)


def exchange(low, high, front, back):
    before, behind = shift(back, "depth", 1), shift(front, "depth", -1)
    return (shift(high, PLANE, 1), shift(low, PLANE, -1), before, behind)


def call(body, outs, operands, scratch=(), limit=16, work=0):
    specs, shapes, results = [], [], []
    for operand, space in operands:
        specs.append(pl.BlockSpec(memory_space=space))
        results.append(operand if space is pl.ANY else pltpu.with_memory_space_constraint(operand, space))
    out_specs = []
    for shape, kind, space in outs:
        out_specs.append(pl.BlockSpec(memory_space=space))
        shapes.append(jax.ShapeDtypeStruct(shape, kind) if space is pl.ANY else space(shape, kind))
    return pl.pallas_call(
        body,
        out_shape=tuple(shapes),
        in_specs=specs,
        out_specs=tuple(out_specs),
        scratch_shapes=list(scratch),
        cost_estimate=pl.CostEstimate(flops=work, bytes_accessed=0, transcendentals=0),
        compiler_params=pltpu.CompilerParams(vmem_limit_bytes=limit * 2**20),
    )(*results)


def sweep(px, py, step):
    group = next(count for count in (7, 6, 5, 4, 3, 2, 1) if (py - 2) % count == 0)
    for p in range(px):
        step(p, 0)

        def several(j, carry):
            for i in range(group):
                step(p, 1 + group * j + i)
            return carry

        lax.fori_loop(0, (py - 2) // group, several, 0)
        step(p, py - 1)


def read_start(start, px, py, cz):
    halves = py // 8

    def body(start_ref, fields_ref, low_ref, high_ref, front_ref, back_ref, raw, sems):
        def copy(chunk):
            p, h = chunk // halves, chunk % halves
            return pltpu.make_async_copy(start_ref.at[:, p, pl.ds(8 * h, 8), :], raw.at[chunk], sems.at[chunk])

        for chunk in range(px * halves):
            copy(chunk).start()

        def step(chunk, carry):
            copy(chunk).wait()
            p, h = chunk // halves, chunk % halves
            rows = pl.multiple_of(8 * h, 8)
            turned = jnp.swapaxes(raw[chunk].astype(f32), 0, 1)
            sent = jnp.concatenate([turned[:, :B], turned[:, 2 * B :]], 1)
            fields_ref[p, pl.ds(rows, 8)] = turned.astype(bf16)

            @pl.when(p == 0)
            def _():
                low_ref[pl.ds(rows, 8)] = sent

            @pl.when(p == px - 1)
            def _():
                high_ref[pl.ds(rows, 8)] = sent

            @pl.when(h == 0)
            def _():
                front_ref[p] = sent[0]

            @pl.when(h == halves - 1)
            def _():
                back_ref[p] = sent[7]

            return carry

        lax.fori_loop(0, px * halves, step, 0)

    plane, row = ((py, 2 * B, cz), f32, VMEM), ((px, 2 * B, cz), f32, VMEM)
    return call(
        body,
        (((px, py, S, cz), bf16, VMEM), plane, plane, row, row),
        ((start, pltpu.HBM),),
        (pltpu.VMEM((px * halves, S, 8, cz), jnp.int32), pltpu.SemaphoreType.DMA((px * halves,))),
    )


def laplace(inside, edges, p, y, at, edge_at, px, py, cz):
    below, above, before, behind = edges
    kept, outer = slice(at, at + B), slice(edge_at, edge_at + B)

    def get(p, y):
        if p < 0:
            row = below[y, outer]
        elif p == px:
            row = above[y, outer]
        elif isinstance(y, int) and y < 0:
            row = before[p, outer]
        elif isinstance(y, int) and y == py:
            row = behind[p, outer]
        else:
            row = inside[p, y, kept]
        return row.astype(inside.dtype)

    center = get(p, y)
    wide = center.astype(f32)
    lane = lax.broadcasted_iota(jnp.int32, (B, cz), 1)
    left = jnp.where(lane == 0, 0.0, pltpu.roll(wide, 1, 1))
    right = jnp.where(lane == cz - 1, 0.0, pltpu.roll(wide, cz - 1, 1))
    beside = (get(p + 1, y) + get(p - 1, y)) + (get(p, y + 1) + get(p, y - 1))
    return 6.0 * wide - (beside.astype(f32) + (left + right))


def set_coefs(labels_ref, coefs, px):
    for p in range(px):
        labels = labels_ref[p]
        for which, table in enumerate((outer_table, damping_table, inner_table)):
            values = [-entry / eps for entry, eps in zip(table, permittivity_table)]
            result = jnp.full(labels.shape, values[0], f32)
            for region in range(1, 4):
                result = jnp.where(labels == region, values[region], result)
            coefs[which, p] = result


def first_lift(labels, fields, gram, edges, px, py, cz):
    def body(labels_ref, fields_ref, gram_ref, below, above, before, behind, lifted, low, high, front, back, coefs):
        set_coefs(labels_ref, coefs, px)
        around = (below, above, before, behind)

        def step(p, y):
            outer, damping, inner = [coefs[k, p, pl.ds(y, 1), :] for k in range(3)]
            middle = fields_ref[p, y, B : 2 * B, :].astype(f32)
            out = (
                outer * laplace(fields_ref, around, p, y, 0, 0, px, py, cz)
                + damping * middle
                + inner * laplace(fields_ref, around, p, y, 2 * B, B, px, py, cz)
            )
            lifted[p, y] = out
            if p in (0, px - 1) or isinstance(y, int):
                edge = jnp.concatenate([out, middle], 0)
            if p == 0:
                low[y] = edge
            if p == px - 1:
                high[y] = edge
            if isinstance(y, int):
                (back if y else front)[p] = edge

        sweep(px, py, step)

    plane, row = ((py, 2 * B, cz), f32, VMEM), ((px, 2 * B, cz), f32, VMEM)
    return call(
        body,
        (((px, py, B, cz), f32, VMEM), plane, plane, row, row),
        ((labels, VMEM), (fields, VMEM), (gram, ANY)) + tuple((edge, VMEM) for edge in edges),
        (pltpu.VMEM((3, px, py, cz), f32),),
        4,
    )


def gram_loop(count, rows, left, right, shape):
    def step(j, total):
        lhs = jnp.concatenate([left(j * count + i) for i in range(count)], 1)
        rhs = jnp.concatenate([right(j * count + i) for i in range(count)], 1)
        return total + lax.dot_general(lhs, rhs, (((1,), (1,)), ((), ())), preferred_element_type=f32)

    return lax.fori_loop(0, rows // count, step, jnp.zeros(shape, f32))


def start_products(fields, px, py):
    def body(fields_ref, gram_ref):
        def row(r):
            return fields_ref[r // py, r % py]

        gram_ref[...] = gram_loop(16, px * py, row, row, (S, S))

    return call(body, (((S, S), f32, VMEM),), ((fields, VMEM),), limit=4, work=10**9)[0]


def split(values):
    high = values.astype(bf16)
    return jnp.concatenate([high, (values - high.astype(f32)).astype(bf16)], 0)


def lifted_products(fields, lifted, px, py, cz):
    def body(fields_ref, lifted_ref, halves_ref, gram_ref):
        def part(r):
            halves = split(lifted_ref[r // py, r % py])
            halves_ref[r // py, r % py] = halves
            return halves

        def step(j, total):
            parts = [part(8 * j + i) for i in range(8)]
            rows = [fields_ref[(8 * j + i) // py, (8 * j + i) % py] for i in range(8)]
            rhs = jnp.concatenate(parts, 1)
            lhs = jnp.concatenate([jnp.concatenate(rows, 1), rhs], 0)
            return total + lax.dot_general(lhs, rhs, (((1,), (1,)), ((), ())), preferred_element_type=f32)

        gram_ref[...] = lax.fori_loop(0, px * py // 8, step, jnp.zeros((S + 2 * B, 2 * B), f32))

    return call(
        body,
        (((px, py, 2 * B, cz), bf16, VMEM), ((S + 2 * B, 2 * B), f32, VMEM)),
        ((fields, VMEM), (lifted, VMEM)),
        limit=4,
        work=10**9,
    )


def second_lift(labels, fields, lifted, ends, halves, grams, px, py, cz):
    def body(labels_ref, fields_ref, lifted_ref, halves_ref, start_ref, middle_ref, *refs):
        end_refs, (parts_out, packed, coefs, parts, sems) = refs[:4], refs[4:]
        set_coefs(labels_ref, coefs, px)

        def copy(p):
            return pltpu.make_async_copy(parts.at[p], parts_out.at[p], sems.at[p])

        def step(p, y):
            outer, damping, inner = [coefs[k, p, pl.ds(y, 1), :] for k in range(3)]
            now = fields_ref[p, y]
            second = (
                outer * laplace(lifted_ref, end_refs, p, y, 0, 0, px, py, cz)
                + damping * now[:B].astype(f32)
                + inner * laplace(fields_ref, end_refs, p, y, B, B, px, py, cz)
            )
            parts[p, y] = jnp.concatenate([now, halves_ref[p, y], split(second)], 0)

        def left(r):
            return parts[r // py, r % py]

        def right(r):
            return parts[r // py, r % py, S + 2 * B :]

        sweep(px, py, step)
        for p in range(px):
            copy(p).start()
        last = gram_loop(8, px * py, left, right, (A, 2 * B))
        last = jnp.concatenate([last, jnp.zeros((A, 128 - 2 * B), f32)], 1)
        last = last + pltpu.roll(last, 128 - B, 1)
        middle = jnp.concatenate([middle_ref[...], jnp.zeros((S + 2 * B, 128 - 2 * B), f32)], 1)
        middle = middle + pltpu.roll(middle, 128 - B, 1)
        middle = jnp.concatenate([middle[:S], middle[S : S + B] + middle[S + B :]], 0)
        last = jnp.concatenate([last[:S], last[S : S + B] + last[S + B : S + 2 * B], last[S + 2 * B : S + 3 * B] + last[S + 3 * B :]], 0)
        first = jnp.concatenate([start_ref[...], jnp.zeros((S, 128 - S), f32)], 1)
        lane = lax.broadcasted_iota(jnp.int32, (B, 128), 1)
        sums = [jnp.zeros((B, 128), f32)] * 2
        for at, (i, j) in enumerate(BLOCKS):
            source, column = (first, j) if j < 3 else ((middle, 0) if j == 3 else (last, 0))
            moved = pltpu.roll(source[B * i : B * i + B], (B * (at % 8 - column)) % 128, 1)
            kept = (lane >= B * (at % 8)) & (lane < B * (at % 8) + B)
            sums[at // 8] = jnp.where(kept, moved, sums[at // 8])
        packed[...] = jnp.concatenate(sums, 0)
        for p in range(px):
            copy(p).wait()

    return call(
        body,
        (((px, py, A, cz), bf16, pltpu.HBM), ((2 * B, 128), f32, VMEM)),
        tuple((x, VMEM) for x in (labels, fields, lifted, halves) + tuple(grams) + ends),
        (
            pltpu.VMEM((3, px, py, cz), f32),
            pltpu.VMEM((px, py, A, cz), bf16),
            pltpu.SemaphoreType.DMA((px,)),
        ),
        12,
    )


def factorize(matrix, count):
    lane = lax.broadcasted_iota(jnp.int32, (8, 128), 1)
    sub = lax.broadcasted_iota(jnp.int32, (8, 128), 0)
    tiles = [matrix[8 * j : 8 * j + 8] for j in range(count // 8)]
    right = [jnp.where(lane == sub + 8 * j, 1.0, 0.0) for j in range(count // 8)]
    upper, inverse = [], []
    for k in range(count):
        own, s = k // 8, k % 8
        pivot = tiles[own][s : s + 1, k : k + 1]
        scale = lax.rsqrt(pivot)
        row = tiles[own][s : s + 1] * scale
        other = right[own][s : s + 1] * scale
        upper.append(row)
        inverse.append(other)
        for j in range(own, count // 8):
            factor = tiles[j][:, k : k + 1] * scale
            if j == own:
                factor = jnp.where(sub[:, :1] > s, factor, 0.0)
            tiles[j] = tiles[j] - factor * row
            right[j] = right[j] - factor * other
    upper = jnp.concatenate(upper, 0)
    inverse = jnp.concatenate(inverse, 0)
    lane = lax.broadcasted_iota(jnp.int32, (count, 128), 1)
    sub = lax.broadcasted_iota(jnp.int32, (count, 128), 0)
    return jnp.where((lane >= sub) & (lane < count), upper, 0.0), inverse


def place(strip, origin, target):
    lane = lax.broadcasted_iota(jnp.int32, strip.shape, 1)
    moved = pltpu.roll(strip, (B * (target - origin)) % 128, 1) if target != origin else strip
    return jnp.where((lane >= B * target) & (lane < B * target + B), moved, 0.0)


def algebra(packed, cells_total):
    def body(packed_ref, matrix_ref, coords_ref):
        table = packed_ref[...] * (1.0 / cells_total)
        rows = [jnp.zeros((B, 128), f32)] * 8
        for at, (i, j) in enumerate(BLOCKS):
            rows[i] = rows[i] + place(table[B * (at // 8) : B * (at // 8) + B], at % 8, j)
        square = jnp.concatenate(rows, 0)
        lane = lax.broadcasted_iota(jnp.int32, (128, 128), 1)
        sub = lax.broadcasted_iota(jnp.int32, (128, 128), 0)
        gram = jnp.where(lane // B >= sub // B, square, square.T)[:V]
        rows = []
        for i in range(3):
            total = jnp.zeros((B, 128), f32)
            for blocks in CHAIN:
                strip = gram[B * blocks[i] : B * blocks[i] + B]
                for j in range(3):
                    total = total + place(strip, blocks[j], j)
            rows.append(total)
        upper, inverse = factorize(gram, V)
        _, small = factorize(jnp.concatenate(rows, 0), S)
        for i in range(3):
            chosen = place(small, 0, CHAIN[i][0]) + place(small, 1, CHAIN[i][1]) + place(small, 2, CHAIN[i][2])
            coords_ref[i] = lax.dot_general(
                chosen, upper, (((1,), (1,)), ((), ())), precision=highest, preferred_element_type=f32
            )
        lane = lax.broadcasted_iota(jnp.int32, (V, 128), 1)
        matrix = jnp.where(lane < S + B, inverse, 0.0)
        matrix = matrix + place(inverse, 3, 4) + place(inverse, 4, 5) + place(inverse, 4, 6)
        matrix = matrix[:, :A]
        high = matrix.astype(bf16)
        matrix_ref[:V] = high
        matrix_ref[V:] = (matrix - high.astype(f32)).astype(bf16)

    return call(
        body,
        (((2 * V, A), bf16, VMEM), ((3, S, V), f32, VMEM)),
        ((packed, VMEM),),
        limit=4,
    )


def write_basis(parts, matrix, px, py, cz):
    halves = py // 8

    def body(parts_in, matrix_ref, out_ref, parts_ref, turned, ready, sems, in_sems):
        weights = matrix_ref[...]

        def fetch(chunk):
            p, h = chunk // halves, chunk % halves
            here = (p, pl.ds(8 * h, 8))
            return pltpu.make_async_copy(parts_in.at[here], parts_ref.at[here], in_sems.at[chunk])

        for chunk in range(px * halves):
            fetch(chunk).start()

        def copy(chunk):
            p, h = chunk // halves, chunk % halves
            return pltpu.make_async_copy(ready.at[chunk], out_ref.at[:, p, pl.ds(8 * h, 8), :], sems.at[chunk])

        def step(chunk, carry):
            p, h = chunk // halves, chunk % halves
            fetch(chunk).wait()
            for y in range(8):
                out = jnp.dot(weights, parts_ref[p, 8 * h + y], preferred_element_type=f32)
                turned[y] = out[:V] + out[V:]
            ready[chunk] = jnp.swapaxes(turned[...], 0, 1)
            copy(chunk).start()
            return carry

        lax.fori_loop(0, px * halves, step, 0)
        for chunk in range(px * halves):
            copy(chunk).wait()

    return call(
        body,
        (((V, px, py, cz), f32, ANY),),
        ((parts, pltpu.HBM), (matrix, VMEM)),
        (
            pltpu.VMEM((px, py, A, cz), bf16),
            pltpu.VMEM((8, V, cz), f32),
            pltpu.VMEM((px * halves, V, 8, cz), f32),
            pltpu.SemaphoreType.DMA((px * halves,)),
            pltpu.SemaphoreType.DMA((px * halves,)),
        ),
        20,
    )[0]


def per_device(labels, start):
    px, py, cz = labels.shape
    cells_total = labels.size * lax.axis_size(PLANE) * lax.axis_size("depth")
    fields, *edges = read_start(start.reshape((S, px, py, cz)), px, py, cz)
    edges = exchange(*edges)
    start_gram = start_products(fields, px, py)
    lifted, *ends = first_lift(labels, fields, start_gram, edges, px, py, cz)
    ends = exchange(*ends)
    halves, middle_gram = lifted_products(fields, lifted, px, py, cz)
    parts, packed = second_lift(labels, fields, lifted, ends, halves, (start_gram, middle_gram), px, py, cz)
    matrix, turned = algebra(sum_all(packed), cells_total)
    return (write_basis(parts, matrix, px, py, cz), jnp.swapaxes(turned, 1, 2))


def solution(mesh):
    finer = Mesh(
        mesh.devices.reshape(4, 8, 2, mesh.shape["depth"]),
        ("plane_0", "plane_1", "plane_2", "depth"),
    )
    return jax.shard_map(
        per_device,
        mesh=finer,
        in_specs=(P(PLANE, "depth", None), P(None, None, PLANE, "depth", None)),
        out_specs=(P(None, PLANE, "depth", None), P()),
        check_vma=False,
    )
```

```python
import itertools

import jax
import jax.numpy as jnp
from jax import lax
from jax.experimental import pallas as pl
from jax.experimental.pallas import tpu as pltpu
from jax.sharding import Mesh
from jax.sharding import PartitionSpec as P

PLANE = ("plane_0", "plane_1", "plane_2")
WIDE = ("plane_1", "depth")
NARROW = ("plane_0", "plane_2")
B = 16
S = 3 * B
V = 5 * B
A = V + 2 * B
GROUP = 8

f32 = jnp.float32
bf16 = jnp.bfloat16
highest = lax.Precision.HIGHEST
permittivity_table = (1.0, 2.5, 4.0, 6.5)
damping_table = (0.3, 1.2, 0.05, 2.0)
outer_table = (1.0, 0.5, 2.0, 0.8)
inner_table = (1.0, 3.0, 0.6, 1.5)
CHAIN = ((0, 3, 4), (1, 0, 3), (2, 1, 0))
BLOCKS = [(i, j) for j in range(5) for i in range(j + 1)]

VMEM = pltpu.VMEM
ANY = pl.ANY


def parities():
    return lax.axis_index("plane_2"), lax.axis_index("depth") % 2


def spread(pieces, copies, halved=False):
    def body(pieces_ref, out_ref):
        total = pieces_ref[0]
        for i in range(1, pieces.shape[0]):
            total = total + pieces_ref[i]
        if halved:
            total = jnp.where(parities()[0] == 0, total[:B], total[B:])
        for i in range(copies):
            out_ref[i] = total

    return call(body, (((copies, B, 128), f32, VMEM),), ((pieces, VMEM),), limit=4)[0]


def sum_all(table):
    both = lax.all_gather(table, "plane_2")
    own = spread(both, lax.axis_size(WIDE), True)
    own = spread(lax.all_to_all(own, WIDE, 0, 0, tiled=True), lax.axis_size(NARROW))
    return lax.all_to_all(own, NARROW, 0, 0, tiled=True)


def swap(edge, axis, first):
    peers = lax.axis_size(axis)
    pairs = [(i, i + 1) for i in range(first, peers - 1, 2)]
    return lax.ppermute(edge, axis, pairs + [(b, a) for a, b in pairs])


def exchange(plane_even, plane_odd, row_even, row_odd):
    out = []
    for edge, axis, first in (
        (plane_even, PLANE, 0), (plane_odd, PLANE, 1), (row_even, "depth", 0), (row_odd, "depth", 1)
    ):
        out.append(swap(edge, axis, first))
    return tuple(out)


def call(body, outs, operands, scratch=(), limit=16, work=0):
    specs, shapes, results = [], [], []
    for operand, space in operands:
        specs.append(pl.BlockSpec(memory_space=space))
        results.append(operand if space is pl.ANY else pltpu.with_memory_space_constraint(operand, space))
    out_specs = []
    for shape, kind, space in outs:
        out_specs.append(pl.BlockSpec(memory_space=space))
        shapes.append(jax.ShapeDtypeStruct(shape, kind) if space is pl.ANY else space(shape, kind))
    return pl.pallas_call(
        body,
        out_shape=tuple(shapes),
        in_specs=specs,
        out_specs=tuple(out_specs),
        scratch_shapes=list(scratch),
        cost_estimate=pl.CostEstimate(flops=work, bytes_accessed=0, transcendentals=0),
        compiler_params=pltpu.CompilerParams(vmem_limit_bytes=limit * 2**20),
    )(*results)


def sweep(px, py, step):
    group = next(count for count in (7, 6, 5, 4, 3, 2, 1) if (py - 2) % count == 0)
    for p in range(px):
        step(p, 0)

        def several(j, carry):
            for i in range(group):
                step(p, 1 + group * j + i)
            return carry

        lax.fori_loop(0, (py - 2) // group, several, 0)
        step(p, py - 1)


def read_start(labels, start, px, py, cz):
    halves = py // 8

    def body(labels_in, start_ref, fields_ref, coefs, plane_even, plane_odd, row_even, row_odd, raw, labels_ref, sems, labels_sem):
        q, r = parities()
        fetch = pltpu.make_async_copy(labels_in, labels_ref, labels_sem)

        def copy(chunk):
            p, h = chunk // halves, chunk % halves
            return pltpu.make_async_copy(start_ref.at[:, p, pl.ds(8 * h, 8), :], raw.at[chunk], sems.at[chunk])

        for chunk in range(px * halves):
            copy(chunk).start()
        fetch.start()

        def step(chunk, carry):
            copy(chunk).wait()
            p, h = chunk // halves, chunk % halves
            rows = pl.multiple_of(8 * h, 8)
            turned = jnp.swapaxes(raw[chunk].astype(f32), 0, 1)
            sent = jnp.concatenate([turned[:, :B], turned[:, 2 * B :]], 1)
            fields_ref[p, pl.ds(rows, 8)] = turned.astype(bf16)

            @pl.when(p == (1 - q) * (px - 1))
            def _():
                plane_even[pl.ds(rows, 8)] = sent

            @pl.when(p == q * (px - 1))
            def _():
                plane_odd[pl.ds(rows, 8)] = sent

            edge = jnp.where(h == 0, sent[0], sent[7])

            @pl.when(h == (1 - r) * (halves - 1))
            def _():
                row_even[p] = edge

            @pl.when(h == r * (halves - 1))
            def _():
                row_odd[p] = edge

            return carry

        lax.fori_loop(0, px * halves, step, 0)
        fetch.wait()
        for p in range(px):
            for which, table in enumerate((outer_table, damping_table, inner_table)):
                coefs[which, p] = coef(labels_ref[p], table)
        plane_even[py, :py] = labels_ref[(1 - q) * (px - 1)].astype(f32)
        plane_odd[py, :py] = labels_ref[q * (px - 1)].astype(f32)
        for p in range(px):
            row_even[px, p : p + 1] = labels_ref[p, pl.ds((1 - r) * (py - 1), 1), :].astype(f32)
            row_odd[px, p : p + 1] = labels_ref[p, pl.ds(r * (py - 1), 1), :].astype(f32)

    plane, row = ((py + 1, 2 * B, cz), f32, VMEM), ((px + 1, 2 * B, cz), f32, VMEM)
    return call(
        body,
        (((px, py, S, cz), bf16, VMEM), ((3, px, py, cz), f32, VMEM), plane, plane, row, row),
        ((labels, pltpu.HBM), (start, pltpu.HBM)),
        (
            pltpu.VMEM((px * halves, S, 8, cz), jnp.int32),
            pltpu.VMEM((px, py, cz), jnp.int32),
            pltpu.SemaphoreType.DMA((px * halves,)),
            pltpu.SemaphoreType.DMA,
        ),
    )


def outside(edges, p, y, px, py):
    plane_even, plane_odd, row_even, row_odd = edges
    q, r = parities()
    if p < 0:
        return jnp.where(q == 0, plane_odd[y], plane_even[y])
    if p == px:
        return jnp.where(q == 0, plane_even[y], plane_odd[y])
    if isinstance(y, int) and y < 0:
        return jnp.where(r == 0, row_odd[p], row_even[p])
    if isinstance(y, int) and y == py:
        return jnp.where(r == 0, row_even[p], row_odd[p])
    return None


def laplace(inside, p, y, at, px, py, cz, edges=None, edge_at=0):
    def get(p, y):
        if 0 <= p < px and (not isinstance(y, int) or 0 <= y < py):
            return [inside[p, y, at : at + B]]
        if edges is None:
            return []
        return [outside(edges, p, y, px, py)[edge_at : edge_at + B].astype(inside.dtype)]

    wide = get(p, y)[0].astype(f32)
    lane = lax.broadcasted_iota(jnp.int32, (B, cz), 1)
    left = jnp.where(lane == 0, 0.0, pltpu.roll(wide, 1, 1))
    right = jnp.where(lane == cz - 1, 0.0, pltpu.roll(wide, cz - 1, 1))
    beside, *others = get(p + 1, y) + get(p - 1, y) + get(p, y + 1) + get(p, y - 1)
    for other in others:
        beside = beside + other
    return 6.0 * wide - (beside.astype(f32) + (left + right))


def coef(labels, table):
    values = [-entry / eps for entry, eps in zip(table, permittivity_table)]
    result = jnp.full(labels.shape, values[0], f32)
    for region in range(1, 4):
        result = jnp.where(labels == region, values[region], result)
    return result


def first_lift(coefs, fields, gram, edges, px, py, cz):
    def body(coefs, fields_ref, gram_ref, *refs):
        around, (lifted, halves, plane_even, plane_odd, row_even, row_odd, theirs) = refs[:4], refs[4:]

        def step(p, y):
            outer, damping, inner = [coefs[k, p, pl.ds(y, 1), :] for k in range(3)]
            middle = fields_ref[p, y, B : 2 * B, :].astype(f32)
            out = (
                outer * laplace(fields_ref, p, y, 0, px, py, cz, around, 0)
                + damping * middle
                + inner * laplace(fields_ref, p, y, 2 * B, px, py, cz, around, B)
            )
            lifted[p, y] = out
            halves[p, y] = split(out)

        sweep(px, py, step)
        q, r = parities()

        for at, received in enumerate(around):
            labels = received[py if at < 2 else px, :py]
            theirs[at, 0], theirs[at, 1] = coef(labels, outer_table), coef(labels, inner_table)

        def edge(at, line, p, y):
            outer, inner = theirs[at, 0, line : line + 1, :], theirs[at, 1, line : line + 1, :]
            return outer * lifted[p, y] + inner * fields_ref[p, y, B : 2 * B, :].astype(f32)

        for y in range(py):
            plane_even[y] = edge(0, y, (1 - q) * (px - 1), y)
            plane_odd[y] = edge(1, y, q * (px - 1), y)
        for p in range(px):
            row_even[p] = edge(2, p, p, (1 - r) * (py - 1))
            row_odd[p] = edge(3, p, p, r * (py - 1))

    plane, row = ((py, B, cz), f32, VMEM), ((px, B, cz), f32, VMEM)
    return call(
        body,
        (((px, py, B, cz), f32, VMEM), ((px, py, 2 * B, cz), bf16, VMEM), plane, plane, row, row),
        ((coefs, VMEM), (fields, VMEM), (gram, ANY)) + tuple((edge, VMEM) for edge in edges),
        (pltpu.VMEM((4, 2, py, cz), f32),),
        4,
    )


def gram_loop(count, rows, left, right, shape):
    def step(j, total):
        lhs = jnp.concatenate([left(j * count + i) for i in range(count)], 1)
        rhs = jnp.concatenate([right(j * count + i) for i in range(count)], 1)
        return total + lax.dot_general(lhs, rhs, (((1,), (1,)), ((), ())), preferred_element_type=f32)

    return lax.fori_loop(0, rows // count, step, jnp.zeros(shape, f32))


def start_products(fields, px, py):
    def body(fields_ref, gram_ref):
        def row(r):
            return fields_ref[r // py, r % py]

        gram_ref[...] = gram_loop(16, px * py, row, row, (S, S))

    return call(body, (((S, S), f32, VMEM),), ((fields, VMEM),), limit=4, work=10**9)[0]


def split(values):
    high = values.astype(bf16)
    return jnp.concatenate([high, (values - high.astype(f32)).astype(bf16)], 0)


def lifted_products(fields, halves, px, py):
    def body(fields_ref, halves_ref, gram_ref):
        def both(r):
            return jnp.concatenate([fields_ref[r // py, r % py], halves_ref[r // py, r % py]], 0)

        def right(r):
            return halves_ref[r // py, r % py]

        gram_ref[...] = gram_loop(8, px * py, both, right, (S + 2 * B, 2 * B))

    return call(
        body,
        (((S + 2 * B, 2 * B), f32, VMEM),),
        ((fields, VMEM), (halves, VMEM)),
        limit=4,
        work=10**9,
    )[0]


def second_lift(coefs, fields, lifted, ends, halves, grams, px, py, cz):
    def body(coefs, fields_ref, lifted_ref, halves_ref, start_ref, middle_ref, *refs):
        end_refs, (parts, packed) = refs[:4], refs[4:]

        def step(p, y):
            outer, damping, inner = [coefs[k, p, pl.ds(y, 1), :] for k in range(3)]
            now = fields_ref[p, y]
            second = (
                outer * laplace(lifted_ref, p, y, 0, px, py, cz)
                + damping * now[:B].astype(f32)
                + inner * laplace(fields_ref, p, y, B, px, py, cz)
            )
            for other in ((p - 1, y), (p + 1, y), (p, y - 1), (p, y + 1)):
                received = outside(end_refs, *other, px, py)
                if received is not None:
                    second = second - received
            parts[p, y] = jnp.concatenate([now, halves_ref[p, y], split(second)], 0)

        def left(r):
            return parts[r // py, r % py]

        def right(r):
            return parts[r // py, r % py, S + 2 * B :]

        sweep(px, py, step)
        last = gram_loop(8, px * py, left, right, (A, 2 * B))
        last = jnp.concatenate([last, jnp.zeros((A, 128 - 2 * B), f32)], 1)
        last = last + pltpu.roll(last, 128 - B, 1)
        middle = jnp.concatenate([middle_ref[...], jnp.zeros((S + 2 * B, 128 - 2 * B), f32)], 1)
        middle = middle + pltpu.roll(middle, 128 - B, 1)
        middle = jnp.concatenate([middle[:S], middle[S : S + B] + middle[S + B :]], 0)
        last = jnp.concatenate([last[:S], last[S : S + B] + last[S + B : S + 2 * B], last[S + 2 * B : S + 3 * B] + last[S + 3 * B :]], 0)
        first = jnp.concatenate([start_ref[...], jnp.zeros((S, 128 - S), f32)], 1)
        lane = lax.broadcasted_iota(jnp.int32, (B, 128), 1)
        sums = [jnp.zeros((B, 128), f32)] * 2
        for at, (i, j) in enumerate(BLOCKS):
            source, column = (first, j) if j < 3 else ((middle, 0) if j == 3 else (last, 0))
            moved = pltpu.roll(source[B * i : B * i + B], (B * (at % 8 - column)) % 128, 1)
            kept = (lane >= B * (at % 8)) & (lane < B * (at % 8) + B)
            sums[at // 8] = jnp.where(kept, moved, sums[at // 8])
        packed[...] = jnp.concatenate(sums, 0)

    return call(
        body,
        (((px, py, A, cz), bf16, VMEM), ((2 * B, 128), f32, VMEM)),
        tuple((x, VMEM) for x in (coefs, fields, lifted, halves) + tuple(grams) + ends),
        limit=4,
    )


def eliminate(matrix, count, found):
    shape = (8, 128)
    lane = lax.broadcasted_iota(jnp.int32, shape, 1)
    sub = lax.broadcasted_iota(jnp.int32, shape, 0)
    tiles = [matrix[8 * j : 8 * j + 8] for j in range(count // 8)]
    right = [jnp.where(lane == sub + 8 * j, 1.0, 0.0) for j in range(count // 8)]
    upper, inverse = [], []

    def row(tile, s):
        return jnp.broadcast_to(tile[s : s + 1], shape)

    for k in range(0, count, GROUP):
        own, s = k // 8, k % 8
        cols = {
            j: [jnp.broadcast_to(tiles[j][:, k + i : k + i + 1], shape) for i in range(GROUP)]
            for j in range(own, count // 8)
        }
        inner = [[row(cols[own][i], s + n) for i in range(n + 1)] for n in range(GROUP)]
        rows = [row(tiles[own], s + n) for n in range(GROUP)]
        others = [row(right[own], s + n) for n in range(GROUP)]
        for i in range(GROUP):
            scale = lax.rsqrt(inner[i][i])
            rows[i], others[i] = rows[i] * scale, others[i] * scale
            factors = {n: inner[n][i] * scale for n in range(i + 1, GROUP)}
            for j in cols:
                cols[j][i] = cols[j][i] * scale
            for n, factor in factors.items():
                for m in range(i + 1, n + 1):
                    inner[n][m] = inner[n][m] - factor * factors[m]
                rows[n] = rows[n] - factor * rows[i]
                others[n] = others[n] - factor * others[i]
                for j in cols:
                    cols[j][n] = cols[j][n] - cols[j][i] * factor
        for i in range(GROUP):
            upper.append(rows[i][:1])
            inverse.append(others[i][:1])
        for j in cols:
            for i in range(GROUP):
                factor = cols[j][i]
                if j == own:
                    factor = jnp.where(sub >= s + GROUP, factor, 0.0)
                tiles[j] = tiles[j] - factor * rows[i]
                right[j] = right[j] - factor * others[i]
        yield
    lane = lax.broadcasted_iota(jnp.int32, (count, 128), 1)
    sub = lax.broadcasted_iota(jnp.int32, (count, 128), 0)
    upper = jnp.concatenate(upper, 0)
    found.append(jnp.where((lane >= sub) & (lane < count), upper, 0.0))
    found.append(jnp.concatenate(inverse, 0))


def factorize(*jobs):
    results = [[] for _ in jobs]
    running = [eliminate(matrix, count, found) for (matrix, count), found in zip(jobs, results)]
    for _ in itertools.zip_longest(*running):
        pass
    return results


def place(strip, origin, target):
    lane = lax.broadcasted_iota(jnp.int32, strip.shape, 1)
    moved = pltpu.roll(strip, (B * (target - origin)) % 128, 1) if target != origin else strip
    return jnp.where((lane >= B * target) & (lane < B * target + B), moved, 0.0)


def finish(packed, parts, cells_total, px, py, cz):
    halves = py // 8

    def body(packed_ref, parts_ref, out_ref, coords_out, turned, ready, coords_ref, sems, coords_sem):
        pieces = [packed_ref[i] for i in range(packed.shape[0])]
        sums = [sum(pieces[c::2][1:], pieces[c]) for c in range(2)]
        table = jnp.concatenate(sums, 0) * (1.0 / cells_total)
        rows = [jnp.zeros((B, 128), f32)] * 8
        for at, (i, j) in enumerate(BLOCKS):
            rows[i] = rows[i] + place(table[B * (at // 8) : B * (at // 8) + B], at % 8, j)
        square = jnp.concatenate(rows, 0)
        lane = lax.broadcasted_iota(jnp.int32, (128, 128), 1)
        sub = lax.broadcasted_iota(jnp.int32, (128, 128), 0)
        gram = jnp.where(lane // B >= sub // B, square, square.T)[:V]
        rows = []
        for i in range(3):
            total = jnp.zeros((B, 128), f32)
            for blocks in CHAIN:
                strip = gram[B * blocks[i] : B * blocks[i] + B]
                for j in range(3):
                    total = total + place(strip, blocks[j], j)
            rows.append(total)
        (upper, inverse), (_, small) = factorize((gram, V), (jnp.concatenate(rows, 0), S))
        lane = lax.broadcasted_iota(jnp.int32, (V, 128), 1)
        matrix = jnp.where(lane < S + B, inverse, 0.0)
        matrix = matrix + place(inverse, 3, 4) + place(inverse, 4, 5) + place(inverse, 4, 6)
        matrix = matrix[:, :A]
        high = matrix.astype(bf16)
        weights = jnp.concatenate([high, (matrix - high.astype(f32)).astype(bf16)], 0)

        def copy(chunk):
            p, h = chunk // halves, chunk % halves
            return pltpu.make_async_copy(ready.at[chunk], out_ref.at[:, p, pl.ds(8 * h, 8), :], sems.at[chunk])

        def step(chunk, carry):
            p, h = chunk // halves, chunk % halves
            for y in range(8):
                out = jnp.dot(weights, parts_ref[p, 8 * h + y], preferred_element_type=f32)
                turned[y] = out[:V] + out[V:]
            ready[chunk] = jnp.swapaxes(turned[...], 0, 1)
            copy(chunk).start()
            return carry

        lax.fori_loop(0, px * halves, step, 0)
        for i in range(3):
            chosen = place(small, 0, CHAIN[i][0]) + place(small, 1, CHAIN[i][1]) + place(small, 2, CHAIN[i][2])
            coords_ref[i] = lax.dot_general(
                chosen, upper, (((1,), (1,)), ((), ())), precision=highest, preferred_element_type=f32
            )
        whole = pltpu.make_async_copy(coords_ref, coords_out, coords_sem)
        whole.start()
        for chunk in range(px * halves):
            copy(chunk).wait()
        whole.wait()

    return call(
        body,
        (((V, px, py, cz), f32, ANY), ((3, S, V), f32, ANY)),
        ((packed, VMEM), (parts, VMEM)),
        (
            pltpu.VMEM((8, V, cz), f32),
            pltpu.VMEM((px * halves, V, 8, cz), f32),
            pltpu.VMEM((3, S, V), f32),
            pltpu.SemaphoreType.DMA((px * halves,)),
            pltpu.SemaphoreType.DMA,
        ),
        16,
    )


def steps(labels, start):
    px, py, cz = labels.shape
    cells_total = labels.size * lax.axis_size(PLANE) * lax.axis_size("depth")
    fields, coefs, *edges = read_start(labels, start.reshape((S, px, py, cz)), px, py, cz)
    edges = exchange(*edges)
    start_gram = start_products(fields, px, py)
    lifted, halves, *ends = first_lift(coefs, fields, start_gram, edges, px, py, cz)
    ends = exchange(*ends)
    middle_gram = lifted_products(fields, halves, px, py)
    parts, packed = second_lift(coefs, fields, lifted, ends, halves, (start_gram, middle_gram), px, py, cz)
    basis_cols, turned = finish(sum_all(packed), parts, cells_total, px, py, cz)
    return (basis_cols, jnp.swapaxes(turned, 1, 2))


def solution(mesh):
    finer = Mesh(
        mesh.devices.reshape(4, 8, 2, mesh.shape["depth"]),
        ("plane_0", "plane_1", "plane_2", "depth"),
    )
    return jax.shard_map(
        steps,
        mesh=finer,
        in_specs=(P(PLANE, "depth", None), P(None, None, PLANE, "depth", None)),
        out_specs=(P(None, PLANE, "depth", None), P()),
        check_vma=False,
    )
```

```python
import itertools

import jax
import jax.numpy as jnp
from jax import lax
from jax.experimental import pallas as pl
from jax.experimental.pallas import tpu as pltpu
from jax.sharding import Mesh
from jax.sharding import PartitionSpec as P

PLANE = ("plane_0", "plane_1", "plane_2")
WIDE = ("plane_1", "depth")
NARROW = ("plane_0", "plane_2")
B = 16
S = 3 * B
V = 5 * B
A = V + 2 * B
GROUP = 8

f32 = jnp.float32
bf16 = jnp.bfloat16
highest = lax.Precision.HIGHEST
permittivity_table = (1.0, 2.5, 4.0, 6.5)
damping_table = (0.3, 1.2, 0.05, 2.0)
outer_table = (1.0, 0.5, 2.0, 0.8)
inner_table = (1.0, 3.0, 0.6, 1.5)
CHAIN = ((0, 3, 4), (1, 0, 3), (2, 1, 0))
BLOCKS = [(i, j) for j in range(5) for i in range(j + 1)]

VMEM = pltpu.VMEM
ANY = pl.ANY


def parities():
    return lax.axis_index("plane_2"), lax.axis_index("depth") % 2


def spread(pieces, copies, halved=False):
    def body(pieces_ref, out_ref):
        total = pieces_ref[0]
        for i in range(1, pieces.shape[0]):
            total = total + pieces_ref[i]
        if halved:
            total = jnp.where(parities()[0] == 0, total[:B], total[B:])
        for i in range(copies):
            out_ref[i] = total

    return call(body, (((copies, B, 128), f32, VMEM),), ((pieces, VMEM),), limit=4)[0]


def sum_all(table):
    both = lax.all_gather(table, "plane_2")
    own = spread(both, lax.axis_size(WIDE), True)
    own = spread(lax.all_to_all(own, WIDE, 0, 0, tiled=True), lax.axis_size(NARROW))
    return lax.all_to_all(own, NARROW, 0, 0, tiled=True)


def swap(edge, axis, first):
    peers = lax.axis_size(axis)
    pairs = [(i, i + 1) for i in range(first, peers - 1, 2)]
    return lax.ppermute(edge, axis, pairs + [(b, a) for a, b in pairs])


def exchange(plane_even, plane_odd, row_even, row_odd):
    return (
        swap(plane_even, PLANE, 0), swap(plane_odd, PLANE, 1), swap(row_even, "depth", 0), swap(row_odd, "depth", 1)
    )


def call(body, outs, operands, scratch=(), limit=16, work=0):
    specs, shapes, results = [], [], []
    for operand, space in operands:
        specs.append(pl.BlockSpec(memory_space=space))
        results.append(operand if space is pl.ANY else pltpu.with_memory_space_constraint(operand, space))
    out_specs = []
    for shape, kind, space in outs:
        out_specs.append(pl.BlockSpec(memory_space=space))
        shapes.append(jax.ShapeDtypeStruct(shape, kind) if space is pl.ANY else space(shape, kind))
    return pl.pallas_call(
        body,
        out_shape=tuple(shapes),
        in_specs=specs,
        out_specs=tuple(out_specs),
        scratch_shapes=list(scratch),
        cost_estimate=pl.CostEstimate(flops=work, bytes_accessed=0, transcendentals=0),
        compiler_params=pltpu.CompilerParams(vmem_limit_bytes=limit * 2**20),
    )(*results)


def sweep(px, py, step, carry):
    group = next(count for count in (7, 6, 5, 4, 3, 2, 1) if (py - 2) % count == 0)
    for p in range(px):
        carry = step(p, (0, py - 1), carry)

        def several(j, value, p=p):
            return step(p, [1 + group * j + i for i in range(group)], value)

        carry = lax.fori_loop(0, (py - 2) // group, several, carry)
    return carry


def read_face(labels, start, px, py, cz):
    halves = py // 8

    def body(labels_in, start_ref, face, raw, labels_ref, sems):
        p = parities()[0] * (px - 1)
        copies = [pltpu.make_async_copy(labels_in.at[p], labels_ref, sems.at[2 * halves])]
        for h in range(halves):
            for i in range(2):
                source = start_ref.at[pl.ds(2 * B * i, B), p, pl.ds(8 * h, 8), :]
                copies.append(pltpu.make_async_copy(source, raw.at[h, pl.ds(B * i, B)], sems.at[2 * h + i]))
        for each in copies:
            each.start()
        for each in copies:
            each.wait()
        for h in range(halves):
            turned = jnp.swapaxes(raw[h].astype(f32), 0, 1)
            for i in range(8):
                face[16 * h + 2 * i] = turned[i, :B]
                face[16 * h + 2 * i + 1] = turned[i, B:]
        face[2 * py, :py] = labels_ref[...].astype(f32)

    return call(
        body,
        (((2 * py + 1, B, cz), f32, VMEM),),
        ((labels, pltpu.HBM), (start, pltpu.HBM)),
        (
            pltpu.VMEM((halves, 2 * B, 8, cz), jnp.int32),
            pltpu.VMEM((py, cz), jnp.int32),
            pltpu.SemaphoreType.DMA((2 * halves + 1,)),
        ),
        4,
    )[0]


def read_start(labels, start, px, py, cz):
    halves = py // 8

    def body(labels_ref, start_ref, fields_ref, coefs, plane_even, row_even, row_odd):
        q, r = parities()


        def step(chunk, carry):
            p, h = chunk // halves, chunk % halves
            rows = pl.multiple_of(8 * h, 8)
            turned = jnp.swapaxes(start_ref[:, p, pl.ds(rows, 8), :].astype(f32), 0, 1)
            fields_ref[p, pl.ds(rows, 8)] = turned.astype(bf16)

            @pl.when(p == (1 - q) * (px - 1))
            def _():
                for i in range(8):
                    plane_even[2 * (rows + i)] = turned[i, :B]
                    plane_even[2 * (rows + i) + 1] = turned[i, 2 * B :]

            edge = jnp.where(h == 0, turned[0], turned[7])

            @pl.when(h == (1 - r) * (halves - 1))
            def _():
                row_even[2 * p] = edge[:B]
                row_even[2 * p + 1] = edge[2 * B :]

            @pl.when(h == r * (halves - 1))
            def _():
                row_odd[2 * p] = edge[:B]
                row_odd[2 * p + 1] = edge[2 * B :]

            return carry

        lax.fori_loop(0, px * halves, step, 0)
        for p in range(px):
            for which, table in enumerate((outer_table, damping_table, inner_table)):
                coefs[which, p] = coef(labels_ref[p], table)
        plane_even[2 * py, :py] = labels_ref[(1 - q) * (px - 1)].astype(f32)
        for p in range(px):
            row_even[2 * px, p : p + 1] = labels_ref[p, pl.ds((1 - r) * (py - 1), 1), :].astype(f32)
            row_odd[2 * px, p : p + 1] = labels_ref[p, pl.ds(r * (py - 1), 1), :].astype(f32)

    plane, row = ((2 * py + 1, B, cz), f32, VMEM), ((2 * px + 1, B, cz), f32, VMEM)
    return call(
        body,
        (((px, py, S, cz), bf16, VMEM), ((3, px, py, cz), f32, VMEM), plane, row, row),
        ((labels, VMEM), (start, VMEM)),
    )


def outside(edges, p, y, px, py, blocks=1, block=0):
    plane_even, plane_odd, row_even, row_odd = edges
    q, r = parities()
    if p < 0:
        first, second, parity, at = plane_odd, plane_even, q, y
    elif p == px:
        first, second, parity, at = plane_even, plane_odd, q, y
    elif isinstance(y, int) and y < 0:
        first, second, parity, at = row_odd, row_even, r, p
    elif isinstance(y, int) and y == py:
        first, second, parity, at = row_even, row_odd, r, p
    else:
        return None
    return jnp.where(parity == 0, first[blocks * at + block], second[blocks * at + block])


def laplace(inside, p, y, at, px, py, cz, edges=None, block=0):
    def get(p, y):
        if 0 <= p < px and (not isinstance(y, int) or 0 <= y < py):
            return [inside[p, y, at : at + B]]
        if edges is None:
            return []
        return [outside(edges, p, y, px, py, 2, block).astype(inside.dtype)]

    wide = get(p, y)[0].astype(f32)
    lane = lax.broadcasted_iota(jnp.int32, (B, cz), 1)
    left = jnp.where(lane == 0, 0.0, pltpu.roll(wide, 1, 1))
    right = jnp.where(lane == cz - 1, 0.0, pltpu.roll(wide, cz - 1, 1))
    beside, *others = get(p + 1, y) + get(p - 1, y) + get(p, y + 1) + get(p, y - 1)
    for other in others:
        beside = beside + other
    return 6.0 * wide - (beside.astype(f32) + (left + right))


def coef(labels, table):
    values = [-entry / eps for entry, eps in zip(table, permittivity_table)]
    result = jnp.full(labels.shape, values[0], f32)
    for region in range(1, 4):
        result = jnp.where(labels == region, values[region], result)
    return result


def first_lift(coefs, fields, gram, edges, px, py, cz):
    def body(coefs, fields_ref, gram_ref, *refs):
        around, (lifted, halves, plane_even, plane_odd, row_even, row_odd, theirs) = refs[:4], refs[4:]

        def step(p, rows, carry):
            for y in rows:
                outer, damping, inner = [coefs[k, p, pl.ds(y, 1), :] for k in range(3)]
                out = (
                    outer * laplace(fields_ref, p, y, 0, px, py, cz, around, 0)
                    + damping * fields_ref[p, y, B : 2 * B, :].astype(f32)
                    + inner * laplace(fields_ref, p, y, 2 * B, px, py, cz, around, 1)
                )
                lifted[p, y] = out
                halves[p, y] = split(out)
            return carry

        sweep(px, py, step, 0)
        q, r = parities()

        for at, received in enumerate(around):
            labels = received[2 * py if at < 2 else 2 * px, :py]
            theirs[at, 0], theirs[at, 1] = coef(labels, outer_table), coef(labels, inner_table)

        def edge(at, line, p, y):
            outer, inner = theirs[at, 0, line : line + 1, :], theirs[at, 1, line : line + 1, :]
            return outer * lifted[p, y] + inner * fields_ref[p, y, B : 2 * B, :].astype(f32)

        for y in range(py):
            plane_even[y] = edge(0, y, (1 - q) * (px - 1), y)
            plane_odd[y] = edge(1, y, q * (px - 1), y)
        for p in range(px):
            row_even[p] = edge(2, p, p, (1 - r) * (py - 1))
            row_odd[p] = edge(3, p, p, r * (py - 1))

    plane, row = ((py, B, cz), f32, VMEM), ((px, B, cz), f32, VMEM)
    return call(
        body,
        (((px, py, B, cz), f32, VMEM), ((px, py, 2 * B, cz), bf16, VMEM), plane, plane, row, row),
        ((coefs, VMEM), (fields, VMEM), (gram, ANY)) + tuple((edge, VMEM) for edge in edges),
        (pltpu.VMEM((4, 2, py, cz), f32),),
        4,
    )


def gram_loop(count, rows, left, right, shape):
    def step(j, total):
        lhs = jnp.concatenate([left(j * count + i) for i in range(count)], 1)
        rhs = jnp.concatenate([right(j * count + i) for i in range(count)], 1)
        return total + lax.dot_general(lhs, rhs, (((1,), (1,)), ((), ())), preferred_element_type=f32)

    return lax.fori_loop(0, rows // count, step, jnp.zeros(shape, f32))


def start_products(fields, px, py):
    def body(fields_ref, gram_ref):
        def row(r):
            return fields_ref[r // py, r % py]

        gram_ref[...] = gram_loop(16, px * py, row, row, (S, S))

    return call(body, (((S, S), f32, VMEM),), ((fields, VMEM),), limit=4, work=10**9)[0]


def split(values):
    high = values.astype(bf16)
    return jnp.concatenate([high, (values - high.astype(f32)).astype(bf16)], 0)


def lifted_products(fields, halves, px, py):
    def body(fields_ref, halves_ref, gram_ref):
        def both(r):
            return jnp.concatenate([fields_ref[r // py, r % py], halves_ref[r // py, r % py]], 0)

        def right(r):
            return halves_ref[r // py, r % py]

        gram_ref[...] = gram_loop(8, px * py, both, right, (S + 2 * B, 2 * B))

    return call(
        body,
        (((S + 2 * B, 2 * B), f32, VMEM),),
        ((fields, VMEM), (halves, VMEM)),
        limit=4,
        work=10**9,
    )[0]


def second_lift(coefs, fields, lifted, ends, halves, grams, px, py, cz):
    def body(coefs, fields_ref, lifted_ref, halves_ref, start_ref, middle_ref, *refs):
        end_refs, (parts, packed) = refs[:4], refs[4:]

        def step(p, rows, gram):
            every = []
            for y in rows:
                outer, damping, inner = [coefs[k, p, pl.ds(y, 1), :] for k in range(3)]
                now = fields_ref[p, y]
                second = (
                    outer * laplace(lifted_ref, p, y, 0, px, py, cz)
                    + damping * now[:B].astype(f32)
                    + inner * laplace(fields_ref, p, y, B, px, py, cz)
                )
                for other in ((p - 1, y), (p + 1, y), (p, y - 1), (p, y + 1)):
                    received = outside(end_refs, *other, px, py)
                    if received is not None:
                        second = second - received
                every.append(jnp.concatenate([now, halves_ref[p, y], split(second)], 0))
                parts[p, y] = every[-1]
            every = jnp.concatenate(every, 1)
            return gram + lax.dot_general(
                every, every[S + 2 * B :], (((1,), (1,)), ((), ())), preferred_element_type=f32
            )

        last = sweep(px, py, step, jnp.zeros((A, 2 * B), f32))
        last = jnp.concatenate([last, jnp.zeros((A, 128 - 2 * B), f32)], 1)
        last = last + pltpu.roll(last, 128 - B, 1)
        middle = jnp.concatenate([middle_ref[...], jnp.zeros((S + 2 * B, 128 - 2 * B), f32)], 1)
        middle = middle + pltpu.roll(middle, 128 - B, 1)
        middle = jnp.concatenate([middle[:S], middle[S : S + B] + middle[S + B :]], 0)
        last = jnp.concatenate([last[:S], last[S : S + B] + last[S + B : S + 2 * B], last[S + 2 * B : S + 3 * B] + last[S + 3 * B :]], 0)
        first = jnp.concatenate([start_ref[...], jnp.zeros((S, 128 - S), f32)], 1)
        lane = lax.broadcasted_iota(jnp.int32, (B, 128), 1)
        sums = [jnp.zeros((B, 128), f32)] * 2
        for at, (i, j) in enumerate(BLOCKS):
            source, column = (first, j) if j < 3 else ((middle, 0) if j == 3 else (last, 0))
            moved = pltpu.roll(source[B * i : B * i + B], (B * (at % 8 - column)) % 128, 1)
            kept = (lane >= B * (at % 8)) & (lane < B * (at % 8) + B)
            sums[at // 8] = jnp.where(kept, moved, sums[at // 8])
        packed[...] = jnp.concatenate(sums, 0)

    return call(
        body,
        (((px, py, A, cz), bf16, VMEM), ((2 * B, 128), f32, VMEM)),
        tuple((x, VMEM) for x in (coefs, fields, lifted, halves) + tuple(grams) + ends),
        limit=4,
    )


def eliminate(matrix, count, found):
    shape = (8, 128)
    lane = lax.broadcasted_iota(jnp.int32, shape, 1)
    sub = lax.broadcasted_iota(jnp.int32, shape, 0)
    tiles = [matrix[8 * j : 8 * j + 8] for j in range(count // 8)]
    right = [jnp.where(lane == sub + 8 * j, 1.0, 0.0) for j in range(count // 8)]
    upper, inverse = [], []

    def row(tile, s):
        return jnp.broadcast_to(tile[s : s + 1], shape)

    for k in range(0, count, GROUP):
        own, s = k // 8, k % 8
        cols = {
            j: [jnp.broadcast_to(tiles[j][:, k + i : k + i + 1], shape) for i in range(GROUP)]
            for j in range(own, count // 8)
        }
        inner = [[row(cols[own][i], s + n) for i in range(n + 1)] for n in range(GROUP)]
        rows = [row(tiles[own], s + n) for n in range(GROUP)]
        others = [row(right[own], s + n) for n in range(GROUP)]
        for i in range(GROUP):
            scale = lax.rsqrt(inner[i][i])
            rows[i], others[i] = rows[i] * scale, others[i] * scale
            factors = {n: inner[n][i] * scale for n in range(i + 1, GROUP)}
            for j in cols:
                cols[j][i] = cols[j][i] * scale
            for n, factor in factors.items():
                for m in range(i + 1, n + 1):
                    inner[n][m] = inner[n][m] - factor * factors[m]
                rows[n] = rows[n] - factor * rows[i]
                others[n] = others[n] - factor * others[i]
                for j in cols:
                    cols[j][n] = cols[j][n] - cols[j][i] * factor
        for i in range(GROUP):
            upper.append(rows[i][:1])
            inverse.append(others[i][:1])
        for j in cols:
            for i in range(GROUP):
                factor = cols[j][i]
                if j == own:
                    factor = jnp.where(sub >= s + GROUP, factor, 0.0)
                tiles[j] = tiles[j] - factor * rows[i]
                right[j] = right[j] - factor * others[i]
        yield
    lane = lax.broadcasted_iota(jnp.int32, (count, 128), 1)
    sub = lax.broadcasted_iota(jnp.int32, (count, 128), 0)
    upper = jnp.concatenate(upper, 0)
    found.append(jnp.where((lane >= sub) & (lane < count), upper, 0.0))
    found.append(jnp.concatenate(inverse, 0))


def factorize(*jobs):
    results = [[] for _ in jobs]
    running = [eliminate(matrix, count, found) for (matrix, count), found in zip(jobs, results)]
    for _ in itertools.zip_longest(*running):
        pass
    return results


def place(strip, origin, target):
    lane = lax.broadcasted_iota(jnp.int32, strip.shape, 1)
    moved = pltpu.roll(strip, (B * (target - origin)) % 128, 1) if target != origin else strip
    return jnp.where((lane >= B * target) & (lane < B * target + B), moved, 0.0)


def finish(packed, parts, cells_total, px, py, cz):
    halves = py // 8

    def body(packed_ref, parts_ref, out_ref, coords_out, ready, coords_ref, sems, coords_sem):
        pieces = [packed_ref[i] for i in range(packed.shape[0])]
        sums = [sum(pieces[c::2][1:], pieces[c]) for c in range(2)]
        table = jnp.concatenate(sums, 0) * (1.0 / cells_total)
        rows = [jnp.zeros((B, 128), f32)] * 8
        for at, (i, j) in enumerate(BLOCKS):
            rows[i] = rows[i] + place(table[B * (at // 8) : B * (at // 8) + B], at % 8, j)
        square = jnp.concatenate(rows, 0)
        lane = lax.broadcasted_iota(jnp.int32, (128, 128), 1)
        sub = lax.broadcasted_iota(jnp.int32, (128, 128), 0)
        gram = jnp.where(lane // B >= sub // B, square, square.T)[:V]
        rows = []
        for i in range(3):
            total = jnp.zeros((B, 128), f32)
            for blocks in CHAIN:
                strip = gram[B * blocks[i] : B * blocks[i] + B]
                for j in range(3):
                    total = total + place(strip, blocks[j], j)
            rows.append(total)
        (upper, inverse), (_, small) = factorize((gram, V), (jnp.concatenate(rows, 0), S))
        lane = lax.broadcasted_iota(jnp.int32, (V, 128), 1)
        matrix = jnp.where(lane < S + B, inverse, 0.0)
        matrix = matrix + place(inverse, 3, 4) + place(inverse, 4, 5) + place(inverse, 4, 6)
        matrix = matrix[:, :A]
        high = matrix.astype(bf16)
        weights = jnp.concatenate([high, (matrix - high.astype(f32)).astype(bf16)], 1)

        def copy(chunk):
            p, h = chunk // halves, chunk % halves
            return pltpu.make_async_copy(ready.at[chunk], out_ref.at[:, p, pl.ds(8 * h, 8), :], sems.at[chunk])

        def step(chunk, carry):
            p, h = chunk // halves, chunk % halves
            for y in range(0, 8, 2):
                part = jnp.concatenate([parts_ref[p, 8 * h + y + i] for i in range(2)], 1)
                out = jnp.dot(weights, jnp.concatenate([part, part], 0), preferred_element_type=f32)
                for i in range(2):
                    ready[chunk, :, y + i, :] = out[:, cz * i : cz * i + cz]
            copy(chunk).start()
            return carry

        lax.fori_loop(0, px * halves, step, 0)
        for i in range(3):
            chosen = place(small, 0, CHAIN[i][0]) + place(small, 1, CHAIN[i][1]) + place(small, 2, CHAIN[i][2])
            coords_ref[i] = lax.dot_general(
                chosen, upper, (((1,), (1,)), ((), ())), precision=highest, preferred_element_type=f32
            )
        whole = pltpu.make_async_copy(coords_ref, coords_out, coords_sem)
        whole.start()
        for chunk in range(px * halves):
            copy(chunk).wait()
        whole.wait()

    return call(
        body,
        (((V, px, py, cz), f32, ANY), ((3, S, V), f32, ANY)),
        ((packed, VMEM), (parts, VMEM)),
        (
            pltpu.VMEM((px * halves, V, 8, cz), f32),
            pltpu.VMEM((3, S, V), f32),
            pltpu.SemaphoreType.DMA((px * halves,)),
            pltpu.SemaphoreType.DMA,
        ),
        16,
    )


def steps(labels, start):
    px, py, cz = labels.shape
    cells_total = labels.size * lax.axis_size(PLANE) * lax.axis_size("depth")
    start = start.reshape((S, px, py, cz))
    face = read_face(labels, start, px, py, cz)
    fields, coefs, plane_even, *rows = read_start(labels, start, px, py, cz)
    edges = exchange(plane_even, face, *rows)
    start_gram = start_products(fields, px, py)
    lifted, halves, *ends = first_lift(coefs, fields, start_gram, edges, px, py, cz)
    ends = exchange(*ends)
    middle_gram = lifted_products(fields, halves, px, py)
    parts, packed = second_lift(coefs, fields, lifted, ends, halves, (start_gram, middle_gram), px, py, cz)
    basis_cols, turned = finish(sum_all(packed), parts, cells_total, px, py, cz)
    return (basis_cols, jnp.swapaxes(turned, 1, 2))


def solution(mesh):
    finer = Mesh(
        mesh.devices.reshape(4, 8, 2, mesh.shape["depth"]),
        ("plane_0", "plane_1", "plane_2", "depth"),
    )
    return jax.shard_map(
        steps,
        mesh=finer,
        in_specs=(P(PLANE, "depth", None), P(None, None, PLANE, "depth", None)),
        out_specs=(P(None, PLANE, "depth", None), P()),
        check_vma=False,
    )
```

```python
import itertools

import jax
import jax.numpy as jnp
from jax import lax
from jax.experimental import pallas as pl
from jax.experimental.pallas import tpu as pltpu
from jax.sharding import Mesh
from jax.sharding import PartitionSpec as P

PLANE = ("plane_0", "plane_1", "plane_2")
WIDE = ("plane_1", "depth")
NARROW = ("plane_0", "plane_2")
B = 16
S = 3 * B
V = 5 * B
A = V + 2 * B
GROUP = 8

f32 = jnp.float32
bf16 = jnp.bfloat16
highest = lax.Precision.HIGHEST
permittivity_table = (1.0, 2.5, 4.0, 6.5)
damping_table = (0.3, 1.2, 0.05, 2.0)
outer_table = (1.0, 0.5, 2.0, 0.8)
inner_table = (1.0, 3.0, 0.6, 1.5)
CHAIN = ((0, 3, 4), (1, 0, 3), (2, 1, 0))
BLOCKS = [(i, j) for j in range(5) for i in range(j + 1)]

VMEM = pltpu.VMEM
ANY = pl.ANY


def parities():
    return lax.axis_index("plane_2"), lax.axis_index("depth") % 2


def spread(pieces, copies, halved=False):
    def body(pieces_ref, out_ref):
        total = pieces_ref[0]
        for i in range(1, pieces.shape[0]):
            total = total + pieces_ref[i]
        if halved:
            total = jnp.where(parities()[0] == 0, total[:B], total[B:])
        for i in range(copies):
            out_ref[i] = total

    return call(body, (((copies, B, 128), f32, VMEM),), ((pieces, VMEM),), limit=4)[0]


def sum_all(table):
    both = lax.all_gather(table, "plane_2")
    own = spread(both, lax.axis_size(WIDE), True)
    own = spread(lax.all_to_all(own, WIDE, 0, 0, tiled=True), lax.axis_size(NARROW))
    return lax.all_to_all(own, NARROW, 0, 0, tiled=True)


def swap(edge, axis, first):
    peers = lax.axis_size(axis)
    pairs = [(i, i + 1) for i in range(first, peers - 1, 2)]
    return lax.ppermute(edge, axis, pairs + [(b, a) for a, b in pairs])


def exchange(plane_even, plane_odd, row_even, row_odd):
    return (
        swap(plane_even, PLANE, 0), swap(plane_odd, PLANE, 1), swap(row_even, "depth", 0), swap(row_odd, "depth", 1)
    )


def call(body, outs, operands, scratch=(), limit=16, work=0, aliases=None):
    specs, shapes, results = [], [], []
    for operand, space in operands:
        specs.append(pl.BlockSpec(memory_space=space))
        results.append(operand if space is pl.ANY else pltpu.with_memory_space_constraint(operand, space))
    out_specs = []
    for shape, kind, space in outs:
        out_specs.append(pl.BlockSpec(memory_space=space))
        shapes.append(jax.ShapeDtypeStruct(shape, kind) if space is pl.ANY else space(shape, kind))
    return pl.pallas_call(
        body,
        out_shape=tuple(shapes),
        in_specs=specs,
        out_specs=tuple(out_specs),
        scratch_shapes=list(scratch),
        input_output_aliases=aliases or {},
        cost_estimate=pl.CostEstimate(flops=work, bytes_accessed=0, transcendentals=0),
        compiler_params=pltpu.CompilerParams(vmem_limit_bytes=limit * 2**20),
    )(*results)


def sweep(px, py, inner, step, carry):
    group = next(count for count in (7, 6, 5, 4, 3, 2, 1) if (py - 2) % count == 0)
    for p in range(px):
        between = 0 < p < px - 1
        if not inner:
            carry = step(p, (0, py - 1), carry)

        def several(j, value, p=p):
            return step(p, [1 + group * j + i for i in range(group)], value)

        if inner == between:
            carry = lax.fori_loop(0, (py - 2) // group, several, carry)
    return carry


def read_face(labels, start, px, py, cz):
    halves = py // 8

    def body(labels_in, start_ref, face, raw, labels_ref, sems):
        p = parities()[0] * (px - 1)
        copies = [pltpu.make_async_copy(labels_in.at[p], labels_ref, sems.at[2 * halves])]
        for h in range(halves):
            for i in range(2):
                source = start_ref.at[pl.ds(2 * B * i, B), p, pl.ds(8 * h, 8), :]
                copies.append(pltpu.make_async_copy(source, raw.at[h, pl.ds(B * i, B)], sems.at[2 * h + i]))
        for each in copies:
            each.start()
        for each in copies:
            each.wait()
        for h in range(halves):
            turned = jnp.swapaxes(raw[h].astype(f32), 0, 1)
            for i in range(8):
                face[16 * h + 2 * i] = turned[i, :B]
                face[16 * h + 2 * i + 1] = turned[i, B:]
        face[2 * py, :py] = labels_ref[...].astype(f32)

    return call(
        body,
        (((2 * py + 1, B, cz), f32, VMEM),),
        ((labels, pltpu.HBM), (start, pltpu.HBM)),
        (
            pltpu.VMEM((halves, 2 * B, 8, cz), jnp.int32),
            pltpu.VMEM((py, cz), jnp.int32),
            pltpu.SemaphoreType.DMA((2 * halves + 1,)),
        ),
        4,
    )[0]


def read_start(labels, start, px, py, cz):
    halves = py // 8

    def body(labels_ref, start_ref, fields_ref, coefs, plane_even, row_even, row_odd):
        q, r = parities()


        def step(chunk, carry):
            p, h = chunk // halves, chunk % halves
            rows = pl.multiple_of(8 * h, 8)
            turned = jnp.swapaxes(start_ref[:, p, pl.ds(rows, 8), :].astype(f32), 0, 1)
            fields_ref[p, pl.ds(rows, 8)] = turned.astype(bf16)

            @pl.when(p == (1 - q) * (px - 1))
            def _():
                for i in range(8):
                    plane_even[2 * (rows + i)] = turned[i, :B]
                    plane_even[2 * (rows + i) + 1] = turned[i, 2 * B :]

            edge = jnp.where(h == 0, turned[0], turned[7])

            @pl.when(h == (1 - r) * (halves - 1))
            def _():
                row_even[2 * p] = edge[:B]
                row_even[2 * p + 1] = edge[2 * B :]

            @pl.when(h == r * (halves - 1))
            def _():
                row_odd[2 * p] = edge[:B]
                row_odd[2 * p + 1] = edge[2 * B :]

            return carry

        lax.fori_loop(0, px * halves, step, 0)
        for p in range(px):
            for which, table in enumerate((outer_table, damping_table, inner_table)):
                coefs[which, p] = coef(labels_ref[p], table)
        plane_even[2 * py, :py] = labels_ref[(1 - q) * (px - 1)].astype(f32)
        for p in range(px):
            row_even[2 * px, p : p + 1] = labels_ref[p, pl.ds((1 - r) * (py - 1), 1), :].astype(f32)
            row_odd[2 * px, p : p + 1] = labels_ref[p, pl.ds(r * (py - 1), 1), :].astype(f32)

    plane, row = ((2 * py + 1, B, cz), f32, VMEM), ((2 * px + 1, B, cz), f32, VMEM)
    return call(
        body,
        (((px, py, S, cz), bf16, VMEM), ((3, px, py, cz), f32, VMEM), plane, row, row),
        ((labels, VMEM), (start, VMEM)),
    )


def outside(edges, p, y, px, py, blocks=1, block=0):
    plane_even, plane_odd, row_even, row_odd = edges
    q, r = parities()
    if p < 0:
        first, second, parity, at = plane_odd, plane_even, q, y
    elif p == px:
        first, second, parity, at = plane_even, plane_odd, q, y
    elif isinstance(y, int) and y < 0:
        first, second, parity, at = row_odd, row_even, r, p
    elif isinstance(y, int) and y == py:
        first, second, parity, at = row_even, row_odd, r, p
    else:
        return None
    return jnp.where(parity == 0, first[blocks * at + block], second[blocks * at + block])


def laplace(inside, p, y, at, px, py, cz, edges=None, block=0):
    def get(p, y):
        if 0 <= p < px and (not isinstance(y, int) or 0 <= y < py):
            return [inside[p, y, at : at + B]]
        if edges is None:
            return []
        return [outside(edges, p, y, px, py, 2, block).astype(inside.dtype)]

    wide = get(p, y)[0].astype(f32)
    lane = lax.broadcasted_iota(jnp.int32, (B, cz), 1)
    left = jnp.where(lane == 0, 0.0, pltpu.roll(wide, 1, 1))
    right = jnp.where(lane == cz - 1, 0.0, pltpu.roll(wide, cz - 1, 1))
    beside, *others = get(p + 1, y) + get(p - 1, y) + get(p, y + 1) + get(p, y - 1)
    for other in others:
        beside = beside + other
    return 6.0 * wide - (beside.astype(f32) + (left + right))


def coef(labels, table):
    values = [-entry / eps for entry, eps in zip(table, permittivity_table)]
    result = jnp.full(labels.shape, values[0], f32)
    for region in range(1, 4):
        result = jnp.where(labels == region, values[region], result)
    return result


def first_rows(coefs, fields_ref, around, lifted, halves, inner, px, py, cz):
    def step(p, rows, carry):
        for y in rows:
            outer, damping, middle = [coefs[k, p, pl.ds(y, 1), :] for k in range(3)]
            out = (
                outer * laplace(fields_ref, p, y, 0, px, py, cz, around, 0)
                + damping * fields_ref[p, y, B : 2 * B, :].astype(f32)
                + middle * laplace(fields_ref, p, y, 2 * B, px, py, cz, around, 1)
            )
            lifted[p, y] = out
            halves[p, y] = split(out)
        return carry

    sweep(px, py, inner, step, 0)


def first_lift_inner(coefs, fields, px, py, cz):
    def body(coefs, fields_ref, lifted, halves):
        first_rows(coefs, fields_ref, None, lifted, halves, True, px, py, cz)

    return call(
        body,
        (((px, py, B, cz), f32, VMEM), ((px, py, 2 * B, cz), bf16, VMEM)),
        ((coefs, VMEM), (fields, VMEM)),
        limit=4,
        work=10**9,
    )


def first_lift(coefs, fields, gram, lifted, halves, edges, px, py, cz):
    def body(coefs, fields_ref, gram_ref, lifted_in, halves_in, *refs):
        around, (lifted, halves, plane_even, plane_odd, row_even, row_odd, theirs) = refs[:4], refs[4:]
        first_rows(coefs, fields_ref, around, lifted, halves, False, px, py, cz)
        q, r = parities()

        for at, received in enumerate(around):
            labels = received[2 * py if at < 2 else 2 * px, :py]
            theirs[at, 0], theirs[at, 1] = coef(labels, outer_table), coef(labels, inner_table)

        def edge(at, line, p, y):
            outer, inner = theirs[at, 0, line : line + 1, :], theirs[at, 1, line : line + 1, :]
            return outer * lifted[p, y] + inner * fields_ref[p, y, B : 2 * B, :].astype(f32)

        for y in range(py):
            plane_even[y] = edge(0, y, (1 - q) * (px - 1), y)
            plane_odd[y] = edge(1, y, q * (px - 1), y)
        for p in range(px):
            row_even[p] = edge(2, p, p, (1 - r) * (py - 1))
            row_odd[p] = edge(3, p, p, r * (py - 1))

    plane, row = ((py, B, cz), f32, VMEM), ((px, B, cz), f32, VMEM)
    return call(
        body,
        (((px, py, B, cz), f32, VMEM), ((px, py, 2 * B, cz), bf16, VMEM), plane, plane, row, row),
        ((coefs, VMEM), (fields, VMEM), (gram, ANY), (lifted, VMEM), (halves, VMEM))
        + tuple((edge, VMEM) for edge in edges),
        (pltpu.VMEM((4, 2, py, cz), f32),),
        4,
        aliases={3: 0, 4: 1},
    )


def gram_loop(count, rows, left, right, shape):
    def step(j, total):
        lhs = jnp.concatenate([left(j * count + i) for i in range(count)], 1)
        rhs = jnp.concatenate([right(j * count + i) for i in range(count)], 1)
        return total + lax.dot_general(lhs, rhs, (((1,), (1,)), ((), ())), preferred_element_type=f32)

    return lax.fori_loop(0, rows // count, step, jnp.zeros(shape, f32))


def start_products(fields, px, py):
    def body(fields_ref, gram_ref):
        def row(r):
            return fields_ref[r // py, r % py]

        gram_ref[...] = gram_loop(16, px * py, row, row, (S, S))

    return call(body, (((S, S), f32, VMEM),), ((fields, VMEM),), limit=4, work=10**9)[0]


def split(values):
    high = values.astype(bf16)
    return jnp.concatenate([high, (values - high.astype(f32)).astype(bf16)], 0)


def lifted_products(fields, halves, px, py):
    def body(fields_ref, halves_ref, gram_ref):
        def both(r):
            return jnp.concatenate([fields_ref[r // py, r % py], halves_ref[r // py, r % py]], 0)

        def right(r):
            return halves_ref[r // py, r % py]

        gram_ref[...] = gram_loop(8, px * py, both, right, (S + 2 * B, 2 * B))

    return call(
        body,
        (((S + 2 * B, 2 * B), f32, VMEM),),
        ((fields, VMEM), (halves, VMEM)),
        limit=4,
        work=10**9,
    )[0]


def second_rows(coefs, fields_ref, lifted_ref, halves_ref, around, parts, inner, px, py, cz):
    def step(p, rows, gram):
        every = []
        for y in rows:
            outer, damping, middle = [coefs[k, p, pl.ds(y, 1), :] for k in range(3)]
            now = fields_ref[p, y]
            second = (
                outer * laplace(lifted_ref, p, y, 0, px, py, cz)
                + damping * now[:B].astype(f32)
                + middle * laplace(fields_ref, p, y, B, px, py, cz)
            )
            for other in ((p - 1, y), (p + 1, y), (p, y - 1), (p, y + 1)):
                received = None if inner else outside(around, *other, px, py)
                if received is not None:
                    second = second - received
            every.append(jnp.concatenate([now, halves_ref[p, y], split(second)], 0))
            parts[p, y] = every[-1]
        every = jnp.concatenate(every, 1)
        return gram + lax.dot_general(
            every, every[S + 2 * B :], (((1,), (1,)), ((), ())), preferred_element_type=f32
        )

    return sweep(px, py, inner, step, jnp.zeros((A, 2 * B), f32))


def second_lift_inner(coefs, fields, lifted, halves, px, py, cz):
    def body(coefs, fields_ref, lifted_ref, halves_ref, parts, gram_ref):
        gram_ref[...] = second_rows(coefs, fields_ref, lifted_ref, halves_ref, None, parts, True, px, py, cz)

    return call(
        body,
        (((px, py, A, cz), bf16, VMEM), ((A, 2 * B), f32, VMEM)),
        tuple((x, VMEM) for x in (coefs, fields, lifted, halves)),
        limit=4,
        work=10**9,
    )


def second_lift(coefs, fields, lifted, ends, halves, parts, grams, px, py, cz):
    def body(coefs, fields_ref, lifted_ref, halves_ref, parts_in, start_ref, middle_ref, inner_ref, *refs):
        end_refs, (parts, packed) = refs[:4], refs[4:]
        last = second_rows(coefs, fields_ref, lifted_ref, halves_ref, end_refs, parts, False, px, py, cz)
        last = last + inner_ref[...]
        last = jnp.concatenate([last, jnp.zeros((A, 128 - 2 * B), f32)], 1)
        last = last + pltpu.roll(last, 128 - B, 1)
        middle = jnp.concatenate([middle_ref[...], jnp.zeros((S + 2 * B, 128 - 2 * B), f32)], 1)
        middle = middle + pltpu.roll(middle, 128 - B, 1)
        middle = jnp.concatenate([middle[:S], middle[S : S + B] + middle[S + B :]], 0)
        last = jnp.concatenate([last[:S], last[S : S + B] + last[S + B : S + 2 * B], last[S + 2 * B : S + 3 * B] + last[S + 3 * B :]], 0)
        first = jnp.concatenate([start_ref[...], jnp.zeros((S, 128 - S), f32)], 1)
        lane = lax.broadcasted_iota(jnp.int32, (B, 128), 1)
        sums = [jnp.zeros((B, 128), f32)] * 2
        for at, (i, j) in enumerate(BLOCKS):
            source, column = (first, j) if j < 3 else ((middle, 0) if j == 3 else (last, 0))
            moved = pltpu.roll(source[B * i : B * i + B], (B * (at % 8 - column)) % 128, 1)
            kept = (lane >= B * (at % 8)) & (lane < B * (at % 8) + B)
            sums[at // 8] = jnp.where(kept, moved, sums[at // 8])
        packed[...] = jnp.concatenate(sums, 0)

    return call(
        body,
        (((px, py, A, cz), bf16, VMEM), ((2 * B, 128), f32, VMEM)),
        tuple((x, VMEM) for x in (coefs, fields, lifted, halves, parts) + tuple(grams) + ends),
        limit=4,
        aliases={4: 0},
    )


def eliminate(matrix, count, found):
    shape = (8, 128)
    lane = lax.broadcasted_iota(jnp.int32, shape, 1)
    sub = lax.broadcasted_iota(jnp.int32, shape, 0)
    tiles = [matrix[8 * j : 8 * j + 8] for j in range(count // 8)]
    right = [jnp.where(lane == sub + 8 * j, 1.0, 0.0) for j in range(count // 8)]
    upper, inverse = [], []

    def row(tile, s):
        return jnp.broadcast_to(tile[s : s + 1], shape)

    for k in range(0, count, GROUP):
        own, s = k // 8, k % 8
        cols = {
            j: [jnp.broadcast_to(tiles[j][:, k + i : k + i + 1], shape) for i in range(GROUP)]
            for j in range(own, count // 8)
        }
        inner = [[row(cols[own][i], s + n) for i in range(n + 1)] for n in range(GROUP)]
        rows = [row(tiles[own], s + n) for n in range(GROUP)]
        others = [row(right[own], s + n) for n in range(GROUP)]
        for i in range(GROUP):
            scale = lax.rsqrt(inner[i][i])
            rows[i], others[i] = rows[i] * scale, others[i] * scale
            factors = {n: inner[n][i] * scale for n in range(i + 1, GROUP)}
            for j in cols:
                cols[j][i] = cols[j][i] * scale
            for n, factor in factors.items():
                for m in range(i + 1, n + 1):
                    inner[n][m] = inner[n][m] - factor * factors[m]
                rows[n] = rows[n] - factor * rows[i]
                others[n] = others[n] - factor * others[i]
                for j in cols:
                    cols[j][n] = cols[j][n] - cols[j][i] * factor
        for i in range(GROUP):
            upper.append(rows[i][:1])
            inverse.append(others[i][:1])
        for j in cols:
            for i in range(GROUP):
                factor = cols[j][i]
                if j == own:
                    factor = jnp.where(sub >= s + GROUP, factor, 0.0)
                tiles[j] = tiles[j] - factor * rows[i]
                right[j] = right[j] - factor * others[i]
        yield
    lane = lax.broadcasted_iota(jnp.int32, (count, 128), 1)
    sub = lax.broadcasted_iota(jnp.int32, (count, 128), 0)
    upper = jnp.concatenate(upper, 0)
    found.append(jnp.where((lane >= sub) & (lane < count), upper, 0.0))
    found.append(jnp.concatenate(inverse, 0))


def factorize(*jobs):
    results = [[] for _ in jobs]
    running = [eliminate(matrix, count, found) for (matrix, count), found in zip(jobs, results)]
    for _ in itertools.zip_longest(*running):
        pass
    return results


def place(strip, origin, target):
    lane = lax.broadcasted_iota(jnp.int32, strip.shape, 1)
    moved = pltpu.roll(strip, (B * (target - origin)) % 128, 1) if target != origin else strip
    return jnp.where((lane >= B * target) & (lane < B * target + B), moved, 0.0)


def finish(packed, parts, cells_total, px, py, cz):
    halves = py // 8

    def body(packed_ref, parts_ref, out_ref, coords_out, ready, coords_ref, sems, coords_sem):
        pieces = [packed_ref[i] for i in range(packed.shape[0])]
        sums = [sum(pieces[c::2][1:], pieces[c]) for c in range(2)]
        table = jnp.concatenate(sums, 0) * (1.0 / cells_total)
        rows = [jnp.zeros((B, 128), f32)] * 8
        for at, (i, j) in enumerate(BLOCKS):
            rows[i] = rows[i] + place(table[B * (at // 8) : B * (at // 8) + B], at % 8, j)
        square = jnp.concatenate(rows, 0)
        lane = lax.broadcasted_iota(jnp.int32, (128, 128), 1)
        sub = lax.broadcasted_iota(jnp.int32, (128, 128), 0)
        gram = jnp.where(lane // B >= sub // B, square, square.T)[:V]
        rows = []
        for i in range(3):
            total = jnp.zeros((B, 128), f32)
            for blocks in CHAIN:
                strip = gram[B * blocks[i] : B * blocks[i] + B]
                for j in range(3):
                    total = total + place(strip, blocks[j], j)
            rows.append(total)
        (upper, inverse), (_, small) = factorize((gram, V), (jnp.concatenate(rows, 0), S))
        lane = lax.broadcasted_iota(jnp.int32, (V, 128), 1)
        matrix = jnp.where(lane < S + B, inverse, 0.0)
        matrix = matrix + place(inverse, 3, 4) + place(inverse, 4, 5) + place(inverse, 4, 6)
        matrix = matrix[:, :A]
        high = matrix.astype(bf16)
        weights = jnp.concatenate([high, (matrix - high.astype(f32)).astype(bf16)], 1)

        def copy(chunk):
            p, h = chunk // halves, chunk % halves
            return pltpu.make_async_copy(ready.at[chunk], out_ref.at[:, p, pl.ds(8 * h, 8), :], sems.at[chunk])

        def step(chunk, carry):
            p, h = chunk // halves, chunk % halves
            for y in range(0, 8, 2):
                part = jnp.concatenate([parts_ref[p, 8 * h + y + i] for i in range(2)], 1)
                out = jnp.dot(weights, jnp.concatenate([part, part], 0), preferred_element_type=f32)
                for i in range(2):
                    ready[chunk, :, y + i, :] = out[:, cz * i : cz * i + cz]
            copy(chunk).start()
            return carry

        lax.fori_loop(0, px * halves, step, 0)
        for i in range(3):
            chosen = place(small, 0, CHAIN[i][0]) + place(small, 1, CHAIN[i][1]) + place(small, 2, CHAIN[i][2])
            coords_ref[i] = lax.dot_general(
                chosen, upper, (((1,), (1,)), ((), ())), precision=highest, preferred_element_type=f32
            )
        whole = pltpu.make_async_copy(coords_ref, coords_out, coords_sem)
        whole.start()
        for chunk in range(px * halves):
            copy(chunk).wait()
        whole.wait()

    return call(
        body,
        (((V, px, py, cz), f32, ANY), ((3, S, V), f32, ANY)),
        ((packed, VMEM), (parts, VMEM)),
        (
            pltpu.VMEM((px * halves, V, 8, cz), f32),
            pltpu.VMEM((3, S, V), f32),
            pltpu.SemaphoreType.DMA((px * halves,)),
            pltpu.SemaphoreType.DMA,
        ),
        16,
    )


def steps(labels, start):
    px, py, cz = labels.shape
    cells_total = labels.size * lax.axis_size(PLANE) * lax.axis_size("depth")
    start = start.reshape((S, px, py, cz))
    face = read_face(labels, start, px, py, cz)
    fields, coefs, plane_even, *rows = read_start(labels, start, px, py, cz)
    edges = exchange(plane_even, face, *rows)
    start_gram = start_products(fields, px, py)
    lifted, halves = first_lift_inner(coefs, fields, px, py, cz)
    lifted, halves, *ends = first_lift(coefs, fields, start_gram, lifted, halves, edges, px, py, cz)
    ends = exchange(*ends)
    middle_gram = lifted_products(fields, halves, px, py)
    parts, inner_gram = second_lift_inner(coefs, fields, lifted, halves, px, py, cz)
    grams = (start_gram, middle_gram, inner_gram)
    parts, packed = second_lift(coefs, fields, lifted, ends, halves, parts, grams, px, py, cz)
    basis_cols, turned = finish(sum_all(packed), parts, cells_total, px, py, cz)
    return (basis_cols, jnp.swapaxes(turned, 1, 2))


def solution(mesh):
    finer = Mesh(
        mesh.devices.reshape(4, 8, 2, mesh.shape["depth"]),
        ("plane_0", "plane_1", "plane_2", "depth"),
    )
    return jax.shard_map(
        steps,
        mesh=finer,
        in_specs=(P(PLANE, "depth", None), P(None, None, PLANE, "depth", None)),
        out_specs=(P(None, PLANE, "depth", None), P()),
        check_vma=False,
    )
```

```python
import itertools

import jax
import jax.numpy as jnp
from jax import lax
from jax.experimental import pallas as pl
from jax.experimental.pallas import tpu as pltpu
from jax.sharding import Mesh
from jax.sharding import PartitionSpec as P

PLANE = ("plane_0", "plane_1", "plane_2")
WIDE = ("plane_1", "depth")
NARROW = ("plane_0", "plane_2")
B = 16
S = 3 * B
V = 5 * B
A = V + 2 * B
GROUP = 8

f32 = jnp.float32
bf16 = jnp.bfloat16
highest = lax.Precision.HIGHEST
permittivity_table = (1.0, 2.5, 4.0, 6.5)
damping_table = (0.3, 1.2, 0.05, 2.0)
outer_table = (1.0, 0.5, 2.0, 0.8)
inner_table = (1.0, 3.0, 0.6, 1.5)
CHAIN = ((0, 3, 4), (1, 0, 3), (2, 1, 0))
BLOCKS = [(i, j) for j in range(5) for i in range(j + 1)]

VMEM = pltpu.VMEM
ANY = pl.ANY


def parities():
    return lax.axis_index("plane_2"), lax.axis_index("depth") % 2


def spread(pieces, copies, halved=False):
    def body(pieces_ref, out_ref):
        total = pieces_ref[0]
        for i in range(1, pieces.shape[0]):
            total = total + pieces_ref[i]
        if halved:
            total = jnp.where(parities()[0] == 0, total[:B], total[B:])
        for i in range(copies):
            out_ref[i] = total

    return call(body, (((copies, B, 128), f32, VMEM),), ((pieces, VMEM),), limit=4)[0]


def sum_all(table):
    both = lax.all_gather(table, "plane_2")
    own = spread(both, lax.axis_size(WIDE), True)
    own = spread(lax.all_to_all(own, WIDE, 0, 0, tiled=True), lax.axis_size(NARROW))
    return lax.all_to_all(own, NARROW, 0, 0, tiled=True)


def swap(edge, axis, first):
    peers = lax.axis_size(axis)
    pairs = [(i, i + 1) for i in range(first, peers - 1, 2)]
    return lax.ppermute(edge, axis, pairs + [(b, a) for a, b in pairs])


def exchange(plane_even, plane_odd, row_even, row_odd):
    return (
        swap(plane_even, PLANE, 0), swap(plane_odd, PLANE, 1), swap(row_even, "depth", 0), swap(row_odd, "depth", 1)
    )


def call(body, outs, operands, scratch=(), limit=16, work=0, aliases=None):
    specs, shapes, results = [], [], []
    for operand, space in operands:
        specs.append(pl.BlockSpec(memory_space=space))
        results.append(operand if space is pl.ANY else pltpu.with_memory_space_constraint(operand, space))
    out_specs = []
    for shape, kind, space in outs:
        out_specs.append(pl.BlockSpec(memory_space=space))
        shapes.append(jax.ShapeDtypeStruct(shape, kind) if space is pl.ANY else space(shape, kind))
    return pl.pallas_call(
        body,
        out_shape=tuple(shapes),
        in_specs=specs,
        out_specs=tuple(out_specs),
        scratch_shapes=list(scratch),
        input_output_aliases=aliases or {},
        cost_estimate=pl.CostEstimate(flops=work, bytes_accessed=0, transcendentals=0),
        compiler_params=pltpu.CompilerParams(vmem_limit_bytes=limit * 2**20),
    )(*results)


def sweep(px, py, inner, step, carry):
    group = next(count for count in (7, 6, 5, 4, 3, 2, 1) if (py - 2) % count == 0)
    for p in range(px):
        between = 0 < p < px - 1
        if not inner:
            carry = step(p, (0, py - 1), carry)

        def several(j, value, p=p):
            return step(p, [1 + group * j + i for i in range(group)], value)

        if inner == between:
            carry = lax.fori_loop(0, (py - 2) // group, several, carry)
    return carry


def read_face(labels, start, px, py, cz):
    halves = py // 8

    def body(labels_in, start_ref, face, raw, labels_ref, sems):
        p = parities()[0] * (px - 1)
        copies = []
        for h in range(halves):
            for i in range(2):
                source = start_ref.at[pl.ds(2 * B * i, B), p, pl.ds(8 * h, 8), :]
                copies.append(pltpu.make_async_copy(source, raw.at[h, pl.ds(B * i, B)], sems.at[2 * h + i]))
        copies.append(pltpu.make_async_copy(labels_in.at[p], labels_ref, sems.at[2 * halves]))
        for each in copies:
            each.start()
        for h in range(halves):
            for j in range(2):
                copies[2 * h + j].wait()
                turned = jnp.swapaxes(raw[h, B * j : B * j + B].astype(f32), 0, 1)
                for i in range(8):
                    face[16 * h + 2 * i + j] = turned[i]
        copies[-1].wait()
        face[2 * py, :py] = labels_ref[...].astype(f32)

    return call(
        body,
        (((2 * py + 1, B, cz), f32, VMEM),),
        ((labels, pltpu.HBM), (start, pltpu.HBM)),
        (
            pltpu.VMEM((halves, 2 * B, 8, cz), jnp.int32),
            pltpu.VMEM((py, cz), jnp.int32),
            pltpu.SemaphoreType.DMA((2 * halves + 1,)),
        ),
        4,
    )[0]


def read_start(labels, start, px, py, cz):
    halves = py // 8

    def body(labels_ref, start_ref, fields_ref, coefs, plane_even, row_even, row_odd):
        q, r = parities()


        def step(chunk, carry):
            p, h = chunk // halves, chunk % halves
            rows = pl.multiple_of(8 * h, 8)
            turned = jnp.swapaxes(start_ref[:, p, pl.ds(rows, 8), :].astype(f32), 0, 1)
            fields_ref[p, pl.ds(rows, 8)] = turned.astype(bf16)

            @pl.when(p == (1 - q) * (px - 1))
            def _():
                for i in range(8):
                    plane_even[2 * (rows + i)] = turned[i, :B]
                    plane_even[2 * (rows + i) + 1] = turned[i, 2 * B :]

            edge = jnp.where(h == 0, turned[0], turned[7])

            @pl.when(h == (1 - r) * (halves - 1))
            def _():
                row_even[2 * p] = edge[:B]
                row_even[2 * p + 1] = edge[2 * B :]

            @pl.when(h == r * (halves - 1))
            def _():
                row_odd[2 * p] = edge[:B]
                row_odd[2 * p + 1] = edge[2 * B :]

            return carry

        lax.fori_loop(0, px * halves, step, 0)
        for p in range(px):
            for which, table in enumerate((outer_table, damping_table, inner_table)):
                coefs[which, p] = coef(labels_ref[p], table)
        plane_even[2 * py, :py] = labels_ref[(1 - q) * (px - 1)].astype(f32)
        for p in range(px):
            row_even[2 * px, p : p + 1] = labels_ref[p, pl.ds((1 - r) * (py - 1), 1), :].astype(f32)
            row_odd[2 * px, p : p + 1] = labels_ref[p, pl.ds(r * (py - 1), 1), :].astype(f32)

    plane, row = ((2 * py + 1, B, cz), f32, VMEM), ((2 * px + 1, B, cz), f32, VMEM)
    return call(
        body,
        (((px, py, S, cz), bf16, VMEM), ((3, px, py, cz), f32, VMEM), plane, row, row),
        ((labels, VMEM), (start, VMEM)),
    )


def outside(edges, p, y, px, py, blocks=1, block=0):
    plane_even, plane_odd, row_even, row_odd = edges
    q, r = parities()
    if p < 0:
        first, second, parity, at = plane_odd, plane_even, q, y
    elif p == px:
        first, second, parity, at = plane_even, plane_odd, q, y
    elif isinstance(y, int) and y < 0:
        first, second, parity, at = row_odd, row_even, r, p
    elif isinstance(y, int) and y == py:
        first, second, parity, at = row_even, row_odd, r, p
    else:
        return None
    return jnp.where(parity == 0, first[blocks * at + block], second[blocks * at + block])


def laplace(inside, p, y, at, px, py, cz, edges=None, block=0):
    def get(p, y):
        if 0 <= p < px and (not isinstance(y, int) or 0 <= y < py):
            return [inside[p, y, at : at + B]]
        if edges is None:
            return []
        return [outside(edges, p, y, px, py, 2, block).astype(inside.dtype)]

    wide = get(p, y)[0].astype(f32)
    lane = lax.broadcasted_iota(jnp.int32, (B, cz), 1)
    left = jnp.where(lane == 0, 0.0, pltpu.roll(wide, 1, 1))
    right = jnp.where(lane == cz - 1, 0.0, pltpu.roll(wide, cz - 1, 1))
    beside, *others = get(p + 1, y) + get(p - 1, y) + get(p, y + 1) + get(p, y - 1)
    for other in others:
        beside = beside + other
    return 6.0 * wide - (beside.astype(f32) + (left + right))


def coef(labels, table):
    values = [-entry / eps for entry, eps in zip(table, permittivity_table)]
    result = jnp.full(labels.shape, values[0], f32)
    for region in range(1, 4):
        result = jnp.where(labels == region, values[region], result)
    return result


def first_rows(coefs, fields_ref, around, lifted, halves, inner, px, py, cz):
    def step(p, rows, carry):
        for y in rows:
            outer, damping, middle = [coefs[k, p, pl.ds(y, 1), :] for k in range(3)]
            out = (
                outer * laplace(fields_ref, p, y, 0, px, py, cz, around, 0)
                + damping * fields_ref[p, y, B : 2 * B, :].astype(f32)
                + middle * laplace(fields_ref, p, y, 2 * B, px, py, cz, around, 1)
            )
            lifted[p, y] = out
            halves[p, y] = split(out)
        return carry

    sweep(px, py, inner, step, 0)


def lifted_rows(fields_ref, halves_ref, inner, px, py):
    def step(p, rows, gram):
        both = jnp.concatenate([jnp.concatenate([fields_ref[p, y], halves_ref[p, y]], 0) for y in rows], 1)
        return gram + lax.dot_general(both, both[S:], (((1,), (1,)), ((), ())), preferred_element_type=f32)

    return sweep(px, py, inner, step, jnp.zeros((S + 2 * B, 2 * B), f32))


def first_lift_inner(coefs, fields, px, py, cz):
    def body(coefs, fields_ref, lifted, halves, gram_ref):
        first_rows(coefs, fields_ref, None, lifted, halves, True, px, py, cz)
        gram_ref[...] = lifted_rows(fields_ref, halves, True, px, py)

    return call(
        body,
        (
            ((px, py, B, cz), f32, VMEM),
            ((px, py, 2 * B, cz), bf16, VMEM),
            ((S + 2 * B, 2 * B), f32, VMEM),
        ),
        ((coefs, VMEM), (fields, VMEM)),
        limit=4,
        work=10**9,
    )


def first_lift(coefs, fields, gram, lifted, halves, edges, px, py, cz):
    def body(coefs, fields_ref, gram_ref, lifted_in, halves_in, *refs):
        around, (lifted, halves, plane_even, plane_odd, row_even, row_odd, theirs) = refs[:4], refs[4:]
        first_rows(coefs, fields_ref, around, lifted, halves, False, px, py, cz)
        q, r = parities()

        for at, received in enumerate(around):
            labels = received[2 * py if at < 2 else 2 * px, :py]
            theirs[at, 0], theirs[at, 1] = coef(labels, outer_table), coef(labels, inner_table)

        def edge(at, line, p, y):
            outer, inner = theirs[at, 0, line : line + 1, :], theirs[at, 1, line : line + 1, :]
            return outer * lifted[p, y] + inner * fields_ref[p, y, B : 2 * B, :].astype(f32)

        for y in range(py):
            plane_even[y] = edge(0, y, (1 - q) * (px - 1), y)
            plane_odd[y] = edge(1, y, q * (px - 1), y)
        for p in range(px):
            row_even[p] = edge(2, p, p, (1 - r) * (py - 1))
            row_odd[p] = edge(3, p, p, r * (py - 1))

    plane, row = ((py, B, cz), f32, VMEM), ((px, B, cz), f32, VMEM)
    return call(
        body,
        (((px, py, B, cz), f32, VMEM), ((px, py, 2 * B, cz), bf16, VMEM), plane, plane, row, row),
        ((coefs, VMEM), (fields, VMEM), (gram, ANY), (lifted, VMEM), (halves, VMEM))
        + tuple((edge, VMEM) for edge in edges),
        (pltpu.VMEM((4, 2, py, cz), f32),),
        4,
        aliases={3: 0, 4: 1},
    )


def gram_loop(count, rows, left, right, shape):
    def step(j, total):
        lhs = jnp.concatenate([left(j * count + i) for i in range(count)], 1)
        rhs = jnp.concatenate([right(j * count + i) for i in range(count)], 1)
        return total + lax.dot_general(lhs, rhs, (((1,), (1,)), ((), ())), preferred_element_type=f32)

    return lax.fori_loop(0, rows // count, step, jnp.zeros(shape, f32))


def start_products(fields, px, py):
    def body(fields_ref, gram_ref):
        def row(r):
            return fields_ref[r // py, r % py]

        gram_ref[...] = gram_loop(16, px * py, row, row, (S, S))

    return call(body, (((S, S), f32, VMEM),), ((fields, VMEM),), limit=4, work=10**9)[0]


def split(values):
    high = values.astype(bf16)
    return jnp.concatenate([high, (values - high.astype(f32)).astype(bf16)], 0)


def lifted_products(fields, halves, px, py):
    def body(fields_ref, halves_ref, gram_ref):
        gram_ref[...] = lifted_rows(fields_ref, halves_ref, False, px, py)

    return call(
        body,
        (((S + 2 * B, 2 * B), f32, VMEM),),
        ((fields, VMEM), (halves, VMEM)),
        limit=4,
        work=10**9,
    )[0]


def second_rows(coefs, fields_ref, lifted_ref, halves_ref, around, parts, inner, px, py, cz):
    def step(p, rows, gram):
        every = []
        for y in rows:
            outer, damping, middle = [coefs[k, p, pl.ds(y, 1), :] for k in range(3)]
            now = fields_ref[p, y]
            second = (
                outer * laplace(lifted_ref, p, y, 0, px, py, cz)
                + damping * now[:B].astype(f32)
                + middle * laplace(fields_ref, p, y, B, px, py, cz)
            )
            for other in ((p - 1, y), (p + 1, y), (p, y - 1), (p, y + 1)):
                received = None if inner else outside(around, *other, px, py)
                if received is not None:
                    second = second - received
            every.append(jnp.concatenate([now, halves_ref[p, y], split(second)], 0))
            parts[p, y] = every[-1]
        every = jnp.concatenate(every, 1)
        return gram + lax.dot_general(
            every, every[S + 2 * B :], (((1,), (1,)), ((), ())), preferred_element_type=f32
        )

    return sweep(px, py, inner, step, jnp.zeros((A, 2 * B), f32))


def second_lift_inner(coefs, fields, lifted, halves, px, py, cz):
    def body(coefs, fields_ref, lifted_ref, halves_ref, parts, gram_ref):
        gram_ref[...] = second_rows(coefs, fields_ref, lifted_ref, halves_ref, None, parts, True, px, py, cz)

    return call(
        body,
        (((px, py, A, cz), bf16, VMEM), ((A, 2 * B), f32, VMEM)),
        tuple((x, VMEM) for x in (coefs, fields, lifted, halves)),
        limit=4,
        work=10**9,
    )


def second_lift(coefs, fields, lifted, ends, halves, parts, grams, px, py, cz):
    def body(coefs, fields_ref, lifted_ref, halves_ref, parts_in, start_ref, middle_ref, within_ref, inner_ref, *refs):
        end_refs, (parts, packed) = refs[:4], refs[4:]
        last = second_rows(coefs, fields_ref, lifted_ref, halves_ref, end_refs, parts, False, px, py, cz)
        last = last + inner_ref[...]
        last = jnp.concatenate([last, jnp.zeros((A, 128 - 2 * B), f32)], 1)
        last = last + pltpu.roll(last, 128 - B, 1)
        middle = jnp.concatenate([middle_ref[...] + within_ref[...], jnp.zeros((S + 2 * B, 128 - 2 * B), f32)], 1)
        middle = middle + pltpu.roll(middle, 128 - B, 1)
        middle = jnp.concatenate([middle[:S], middle[S : S + B] + middle[S + B :]], 0)
        last = jnp.concatenate([last[:S], last[S : S + B] + last[S + B : S + 2 * B], last[S + 2 * B : S + 3 * B] + last[S + 3 * B :]], 0)
        first = jnp.concatenate([start_ref[...], jnp.zeros((S, 128 - S), f32)], 1)
        lane = lax.broadcasted_iota(jnp.int32, (B, 128), 1)
        sums = [jnp.zeros((B, 128), f32)] * 2
        for at, (i, j) in enumerate(BLOCKS):
            source, column = (first, j) if j < 3 else ((middle, 0) if j == 3 else (last, 0))
            moved = pltpu.roll(source[B * i : B * i + B], (B * (at % 8 - column)) % 128, 1)
            kept = (lane >= B * (at % 8)) & (lane < B * (at % 8) + B)
            sums[at // 8] = jnp.where(kept, moved, sums[at // 8])
        packed[...] = jnp.concatenate(sums, 0)

    return call(
        body,
        (((px, py, A, cz), bf16, VMEM), ((2 * B, 128), f32, VMEM)),
        tuple((x, VMEM) for x in (coefs, fields, lifted, halves, parts) + tuple(grams) + ends),
        limit=4,
        aliases={4: 0},
    )


def eliminate(matrix, count, found):
    shape = (8, 128)
    lane = lax.broadcasted_iota(jnp.int32, shape, 1)
    sub = lax.broadcasted_iota(jnp.int32, shape, 0)
    tiles = [matrix[8 * j : 8 * j + 8] for j in range(count // 8)]
    right = [jnp.where(lane == sub + 8 * j, 1.0, 0.0) for j in range(count // 8)]
    upper, inverse = [], []

    def row(tile, s):
        return jnp.broadcast_to(tile[s : s + 1], shape)

    for k in range(0, count, GROUP):
        own, s = k // 8, k % 8
        cols = {
            j: [jnp.broadcast_to(tiles[j][:, k + i : k + i + 1], shape) for i in range(GROUP)]
            for j in range(own, count // 8)
        }
        inner = [[row(cols[own][i], s + n) for i in range(n + 1)] for n in range(GROUP)]
        rows = [row(tiles[own], s + n) for n in range(GROUP)]
        others = [row(right[own], s + n) for n in range(GROUP)]
        for i in range(GROUP):
            scale = lax.rsqrt(inner[i][i])
            rows[i], others[i] = rows[i] * scale, others[i] * scale
            factors = {n: inner[n][i] * scale for n in range(i + 1, GROUP)}
            for j in cols:
                cols[j][i] = cols[j][i] * scale
            for n, factor in factors.items():
                for m in range(i + 1, n + 1):
                    inner[n][m] = inner[n][m] - factor * factors[m]
                rows[n] = rows[n] - factor * rows[i]
                others[n] = others[n] - factor * others[i]
                for j in cols:
                    cols[j][n] = cols[j][n] - cols[j][i] * factor
        for i in range(GROUP):
            upper.append(rows[i][:1])
            inverse.append(others[i][:1])
        for j in cols:
            for i in range(GROUP):
                factor = cols[j][i]
                if j == own:
                    factor = jnp.where(sub >= s + GROUP, factor, 0.0)
                tiles[j] = tiles[j] - factor * rows[i]
                right[j] = right[j] - factor * others[i]
        yield
    lane = lax.broadcasted_iota(jnp.int32, (count, 128), 1)
    sub = lax.broadcasted_iota(jnp.int32, (count, 128), 0)
    upper = jnp.concatenate(upper, 0)
    found.append(jnp.where((lane >= sub) & (lane < count), upper, 0.0))
    found.append(jnp.concatenate(inverse, 0))


def factorize(*jobs):
    results = [[] for _ in jobs]
    running = [eliminate(matrix, count, found) for (matrix, count), found in zip(jobs, results)]
    for _ in itertools.zip_longest(*running):
        pass
    return results


def place(strip, origin, target):
    lane = lax.broadcasted_iota(jnp.int32, strip.shape, 1)
    moved = pltpu.roll(strip, (B * (target - origin)) % 128, 1) if target != origin else strip
    return jnp.where((lane >= B * target) & (lane < B * target + B), moved, 0.0)


def finish(packed, parts, cells_total, px, py, cz):
    halves = py // 8

    def body(packed_ref, parts_ref, out_ref, coords_out, ready, coords_ref, sems, coords_sem):
        pieces = [packed_ref[i] for i in range(packed.shape[0])]
        sums = [sum(pieces[c::2][1:], pieces[c]) for c in range(2)]
        table = jnp.concatenate(sums, 0) * (1.0 / cells_total)
        rows = [jnp.zeros((B, 128), f32)] * 8
        for at, (i, j) in enumerate(BLOCKS):
            rows[i] = rows[i] + place(table[B * (at // 8) : B * (at // 8) + B], at % 8, j)
        square = jnp.concatenate(rows, 0)
        lane = lax.broadcasted_iota(jnp.int32, (128, 128), 1)
        sub = lax.broadcasted_iota(jnp.int32, (128, 128), 0)
        gram = jnp.where(lane // B >= sub // B, square, square.T)[:V]
        rows = []
        for i in range(3):
            total = jnp.zeros((B, 128), f32)
            for blocks in CHAIN:
                strip = gram[B * blocks[i] : B * blocks[i] + B]
                for j in range(3):
                    total = total + place(strip, blocks[j], j)
            rows.append(total)
        (upper, inverse), (_, small) = factorize((gram, V), (jnp.concatenate(rows, 0), S))
        lane = lax.broadcasted_iota(jnp.int32, (V, 128), 1)
        matrix = jnp.where(lane < S + B, inverse, 0.0)
        matrix = matrix + place(inverse, 3, 4) + place(inverse, 4, 5) + place(inverse, 4, 6)
        matrix = matrix[:, :A]
        high = matrix.astype(bf16)
        low = (matrix - high.astype(f32)).astype(bf16)
        weights = jnp.concatenate([high, low[:, : S + B], low[:, S + 2 * B : S + 3 * B]], 1)

        def copy(chunk):
            p, h = chunk // halves, chunk % halves
            return pltpu.make_async_copy(ready.at[chunk], out_ref.at[:, p, pl.ds(8 * h, 8), :], sems.at[chunk])

        def step(chunk, carry):
            p, h = chunk // halves, chunk % halves
            for y in range(0, 8, 2):
                part = jnp.concatenate([parts_ref[p, 8 * h + y + i] for i in range(2)], 1)
                out = jnp.dot(weights, jnp.concatenate([part, part[: S + B], part[S + 2 * B : S + 3 * B]], 0), preferred_element_type=f32)
                for i in range(2):
                    ready[chunk, :, y + i, :] = out[:, cz * i : cz * i + cz]
            copy(chunk).start()
            return carry

        lax.fori_loop(0, px * halves, step, 0)
        for i in range(3):
            chosen = place(small, 0, CHAIN[i][0]) + place(small, 1, CHAIN[i][1]) + place(small, 2, CHAIN[i][2])
            coords_ref[i] = lax.dot_general(
                chosen, upper, (((1,), (1,)), ((), ())), precision=highest, preferred_element_type=f32
            )
        whole = pltpu.make_async_copy(coords_ref, coords_out, coords_sem)
        whole.start()
        for chunk in range(px * halves):
            copy(chunk).wait()
        whole.wait()

    return call(
        body,
        (((V, px, py, cz), f32, ANY), ((3, S, V), f32, ANY)),
        ((packed, VMEM), (parts, VMEM)),
        (
            pltpu.VMEM((px * halves, V, 8, cz), f32),
            pltpu.VMEM((3, S, V), f32),
            pltpu.SemaphoreType.DMA((px * halves,)),
            pltpu.SemaphoreType.DMA,
        ),
        16,
    )


def steps(labels, start):
    px, py, cz = labels.shape
    cells_total = labels.size * lax.axis_size(PLANE) * lax.axis_size("depth")
    start = start.reshape((S, px, py, cz))
    face = read_face(labels, start, px, py, cz)
    fields, coefs, plane_even, *rows = read_start(labels, start, px, py, cz)
    edges = exchange(plane_even, face, *rows)
    start_gram = start_products(fields, px, py)
    lifted, halves, within_gram = first_lift_inner(coefs, fields, px, py, cz)
    lifted, halves, *ends = first_lift(coefs, fields, start_gram, lifted, halves, edges, px, py, cz)
    ends = exchange(*ends)
    middle_gram = lifted_products(fields, halves, px, py)
    parts, inner_gram = second_lift_inner(coefs, fields, lifted, halves, px, py, cz)
    grams = (start_gram, middle_gram, within_gram, inner_gram)
    parts, packed = second_lift(coefs, fields, lifted, ends, halves, parts, grams, px, py, cz)
    basis_cols, turned = finish(sum_all(packed), parts, cells_total, px, py, cz)
    return (basis_cols, jnp.swapaxes(turned, 1, 2))


def solution(mesh):
    finer = Mesh(
        mesh.devices.reshape(4, 8, 2, mesh.shape["depth"]),
        ("plane_0", "plane_1", "plane_2", "depth"),
    )
    return jax.shard_map(
        steps,
        mesh=finer,
        in_specs=(P(PLANE, "depth", None), P(None, None, PLANE, "depth", None)),
        out_specs=(P(None, PLANE, "depth", None), P()),
        check_vma=False,
    )
```
